32 devices in a mesh: prompts: 2 (over x), model: 4 (over z), resp: 4 (over y, core).
Axes of the slice: x: 2, y: 2, z: 4, core: 2. Of those that a mesh axis runs over, the one named last changes fastest.
Arguments:
- x_prompt: bfloat16 [4096, 2560], P(('prompts', 'resp')), parts along dimension 0
- x_resp: bfloat16 [8, 1024, 2560], P(('prompts', 'resp')), parts along dimension 0
- targets: int32 [8, 1024], P(('prompts', 'resp')), parts along dimension 0
- resp_lens: int32 [8], P(('prompts', 'resp')), parts along dimension 0
- attn_gain: float32 [2, 2560], replicated
- w_query: bfloat16 [2, 2560, 20, 128], P(None, None, 'model')
- w_key: bfloat16 [2, 2560, 20, 128], P(None, None, 'model')
- w_value: bfloat16 [2, 2560, 20, 128], P(None, None, 'model')
- w_out: bfloat16 [2, 20, 128, 2560], P(None, 'model')
- mlp_gain: float32 [2, 2560], replicated
- w_gate: bfloat16 [2, 2560, 6912], P(None, None, 'model')
- w_up: bfloat16 [2, 2560, 6912], P(None, None, 'model')
- w_down: bfloat16 [2, 6912, 2560], P(None, 'model')
- final_gain: float32 [2560], replicated
- w_vocab: bfloat16 [2560, 65536], P(None, 'model')
Outputs:
- output: float32 [8, 1024], P(('prompts', 'resp')), parts along dimension 0
There are 2 independent parts. The reference program is written for one: setup_inputs(seed, part) draws one part's arguments, and reference() takes and returns one part's arrays. A program takes and returns all parts, laid end to end along the dimension named above; an argument that names none is the same for every part.
All inputs are finite; a program needn't handle non-finite values.
Results may differ from the reference program's by a relative error of at most 0.00229753.
Values are sent between devices in bfloat16 or wider.
A program may use at most 1 GiB of HBM per device.

```python
import jax
import jax.numpy as jnp
from jax import lax

MODEL_DIM = 2560
NUM_HEADS = 20
KV_HEADS = 20
HEAD_DIM = 128
FFN_DIM = 6912
VOCAB_SIZE = 65536
GROUP_SIZE = 4
PROMPT_ROWS = 512
RESP_LEN = 1024
LAYERS = 2
PROMPT_LEN = GROUP_SIZE * PROMPT_ROWS
EPS = 1e-6
ROPE_BASE = 10000.0


def rms_norm(acts_in, gain_vec):
    acts_f = acts_in.astype(jnp.float32)
    inv_rms = lax.rsqrt(jnp.mean(acts_f * acts_f, axis=-1, keepdims=True) + EPS)
    return (acts_f * inv_rms * gain_vec).astype(jnp.bfloat16)


def rotary(projected, positions):
    half_dim = projected.shape[-1] // 2
    frequency = ROPE_BASE ** (-jnp.arange(half_dim, dtype=jnp.float32) / half_dim)
    angles = positions.astype(jnp.float32)[..., None] * frequency
    cos_part = jnp.cos(angles)[..., None, :]
    sin_part = jnp.sin(angles)[..., None, :]
    lower_half = projected[..., :half_dim]
    upper_half = projected[..., half_dim:]
    return jnp.concatenate([lower_half * cos_part - upper_half * sin_part, upper_half * cos_part + lower_half * sin_part], axis=-1)


def attend(queries, keys, values, query_pos, key_pos):
    tokens = queries.shape[0]
    grouped = queries.reshape(tokens, KV_HEADS, NUM_HEADS // KV_HEADS, HEAD_DIM).astype(jnp.float32)
    scores = jnp.einsum('tkrd,skd->krts', grouped, keys.astype(jnp.float32)) * (HEAD_DIM ** -0.5)
    visible = key_pos[None, :] <= query_pos[:, None]
    scores = jnp.where(visible, scores, -jnp.inf)
    row_max = jnp.max(scores, axis=-1, keepdims=True)
    exp_scores = jnp.exp(scores - row_max)
    row_sum = jnp.moveaxis(jnp.sum(exp_scores, axis=-1), -1, 0)
    mixed = jnp.einsum('krts,skd->tkrd', exp_scores.astype(jnp.bfloat16).astype(jnp.float32), values.astype(jnp.float32))
    return (mixed / row_sum[..., None]).reshape(tokens, NUM_HEADS * HEAD_DIM).astype(jnp.bfloat16)


def setup_inputs(seed: int = 0, part: int = 0) -> dict:
    root_keys = jax.random.split(jax.random.key(seed), 2)
    part_keys = jax.random.split(jax.random.fold_in(root_keys[0], part), 7)
    shared_keys = jax.random.split(root_keys[1], 11)

    def normal_weight(key_in, shape, scale):
        return (jax.random.normal(key_in, shape, jnp.float32) * scale).astype(jnp.bfloat16)

    def gain_draw(key_in, shape):
        return jax.random.uniform(key_in, shape, jnp.float32, 0.25, 1.75)

    topics = jax.random.normal(part_keys[0], (4, 1, MODEL_DIM), jnp.float32)
    prompt_noise = jax.random.normal(part_keys[1], (4, PROMPT_LEN // 4, MODEL_DIM), jnp.float32)
    x_prompt = (0.6 * topics + 0.3 * prompt_noise).reshape(PROMPT_LEN, MODEL_DIM).astype(jnp.bfloat16)
    resp_topics = jax.random.normal(part_keys[2], (GROUP_SIZE, 1, MODEL_DIM), jnp.float32)
    resp_noise = jax.random.normal(part_keys[3], (GROUP_SIZE, RESP_LEN, MODEL_DIM), jnp.float32)
    x_resp = (0.6 * resp_topics + 0.3 * resp_noise).astype(jnp.bfloat16)
    targets = jax.random.randint(part_keys[4], (GROUP_SIZE, RESP_LEN), 0, VOCAB_SIZE, dtype=jnp.int32)
    targets = targets.at[0, 0].set(0).at[0, 1].set(VOCAB_SIZE - 1)
    drawn_lens = jax.random.randint(part_keys[5], (GROUP_SIZE,), RESP_LEN // 8, RESP_LEN + 1, dtype=jnp.int32)
    full_slot = jax.random.randint(part_keys[6], (), 0, GROUP_SIZE, dtype=jnp.int32)
    resp_lens = jnp.where(jnp.arange(GROUP_SIZE) == full_slot, RESP_LEN, drawn_lens).astype(jnp.int32)
    return {
        'x_prompt': x_prompt,
        'x_resp': x_resp,
        'targets': targets,
        'resp_lens': resp_lens,
        'attn_gain': gain_draw(shared_keys[0], (LAYERS, MODEL_DIM)),
        'w_query': normal_weight(shared_keys[1], (LAYERS, MODEL_DIM, NUM_HEADS, HEAD_DIM), MODEL_DIM ** -0.5),
        'w_key': normal_weight(shared_keys[2], (LAYERS, MODEL_DIM, KV_HEADS, HEAD_DIM), MODEL_DIM ** -0.5),
        'w_value': normal_weight(shared_keys[3], (LAYERS, MODEL_DIM, KV_HEADS, HEAD_DIM), MODEL_DIM ** -0.5),
        'w_out': normal_weight(shared_keys[4], (LAYERS, NUM_HEADS, HEAD_DIM, MODEL_DIM), (NUM_HEADS * HEAD_DIM) ** -0.5),
        'mlp_gain': gain_draw(shared_keys[5], (LAYERS, MODEL_DIM)),
        'w_gate': normal_weight(shared_keys[6], (LAYERS, MODEL_DIM, FFN_DIM), MODEL_DIM ** -0.5),
        'w_up': normal_weight(shared_keys[7], (LAYERS, MODEL_DIM, FFN_DIM), MODEL_DIM ** -0.5),
        'w_down': normal_weight(shared_keys[8], (LAYERS, FFN_DIM, MODEL_DIM), FFN_DIM ** -0.5),
        'final_gain': gain_draw(shared_keys[9], (MODEL_DIM,)),
        'w_vocab': normal_weight(shared_keys[10], (MODEL_DIM, VOCAB_SIZE), 2.0 * MODEL_DIM ** -0.5),
    }


def reference(x_prompt, x_resp, targets, resp_lens, attn_gain, w_query, w_key, w_value, w_out, mlp_gain, w_gate, w_up, w_down, final_gain, w_vocab):
    prompt_pos = jnp.arange(PROMPT_LEN)
    resp_pos = PROMPT_LEN + jnp.arange(RESP_LEN)
    key_pos = jnp.concatenate([prompt_pos, resp_pos])

    def project(hidden, weight, heads):
        flat = jnp.dot(hidden, weight.reshape(MODEL_DIM, heads * HEAD_DIM), preferred_element_type=jnp.float32)
        return flat.reshape(hidden.shape[0], heads, HEAD_DIM)

    def key_value(hidden, layer_idx, positions):
        keys = rotary(project(hidden, w_key[layer_idx], KV_HEADS), positions).astype(jnp.bfloat16)
        values = project(hidden, w_value[layer_idx], KV_HEADS).astype(jnp.bfloat16)
        return keys, values

    def query_proj(hidden, layer_idx, positions):
        return rotary(project(hidden, w_query[layer_idx], NUM_HEADS), positions).astype(jnp.bfloat16)

    def finish(residual, mixed, layer_idx):
        attn_out = jnp.dot(mixed, w_out[layer_idx].reshape(NUM_HEADS * HEAD_DIM, MODEL_DIM), preferred_element_type=jnp.float32)
        residual = (residual.astype(jnp.float32) + attn_out).astype(jnp.bfloat16)
        hidden = rms_norm(residual, mlp_gain[layer_idx])
        gate = jnp.dot(hidden, w_gate[layer_idx], preferred_element_type=jnp.float32)
        up_proj = jnp.dot(hidden, w_up[layer_idx], preferred_element_type=jnp.float32)
        inner = (jax.nn.silu(gate) * up_proj).astype(jnp.bfloat16)
        down_out = jnp.dot(inner, w_down[layer_idx], preferred_element_type=jnp.float32)
        return (residual.astype(jnp.float32) + down_out).astype(jnp.bfloat16)

    residual = x_prompt
    prompt_cache = []
    for layer_idx in range(LAYERS):
        hidden = rms_norm(residual, attn_gain[layer_idx])
        keys, values = key_value(hidden, layer_idx, prompt_pos)
        prompt_cache.append((keys, values))
        if layer_idx < LAYERS - 1:
            blocks = query_proj(hidden, layer_idx, prompt_pos).reshape(GROUP_SIZE, PROMPT_ROWS, NUM_HEADS, HEAD_DIM)
            block_pos = prompt_pos.reshape(GROUP_SIZE, PROMPT_ROWS)
            mixed = lax.map(lambda block_args: attend(block_args[0], keys, values, block_args[1], prompt_pos), (blocks, block_pos))
            residual = finish(residual, mixed.reshape(PROMPT_LEN, NUM_HEADS * HEAD_DIM), layer_idx)

    def one_response(resp_args):
        residual_r, target_row, length = resp_args
        for layer_idx in range(LAYERS):
            hidden = rms_norm(residual_r, attn_gain[layer_idx])
            keys, values = key_value(hidden, layer_idx, resp_pos)
            queries = query_proj(hidden, layer_idx, resp_pos)
            all_keys = jnp.concatenate([prompt_cache[layer_idx][0], keys], axis=0)
            all_values = jnp.concatenate([prompt_cache[layer_idx][1], values], axis=0)
            mixed = attend(queries, all_keys, all_values, resp_pos, key_pos)
            residual_r = finish(residual_r, mixed, layer_idx)
        logits = jnp.dot(rms_norm(residual_r, final_gain), w_vocab, preferred_element_type=jnp.float32)
        picked = jnp.take_along_axis(logits, target_row[:, None], axis=-1)[:, 0]
        log_probs = picked - jax.nn.logsumexp(logits, axis=-1)
        return jnp.where(jnp.arange(RESP_LEN) < length, log_probs, 0.0)

    return lax.map(one_response, (x_resp, targets, resp_lens))
```

```python
import functools

import jax
import jax.numpy as jnp
from jax import lax
from jax.experimental import pallas as pl
from jax.experimental.pallas import tpu as pltpu
from jax.sharding import PartitionSpec as P

EPS = 1e-6
ROPE_BASE = 10000.0
LOG2E = 1.4426950408889634
HD = 128
NEG = -1e30
ANY = pl.BlockSpec(memory_space=pl.ANY)
SMEM = pl.BlockSpec(memory_space=pltpu.SMEM)
VMEM = pl.BlockSpec(memory_space=pltpu.VMEM)
VLIMIT = 60 * 1024 * 1024


def params(**kw):
    return pltpu.CompilerParams(vmem_limit_bytes=VLIMIT, **kw)


def cost(flops, nbytes, trans=0):
    return pl.CostEstimate(flops=int(flops), bytes_accessed=int(nbytes), transcendentals=int(trans))


def norm_rows(x, gain):
    x = x.astype(jnp.float32)
    inv = lax.rsqrt(jnp.mean(x * x, axis=-1, keepdims=True) + EPS)
    return (x * inv * gain).astype(jnp.bfloat16)


def start_pieces(z, pieces, dst, sems, axis):
    own, rest = pieces[0], pieces[1:]
    size = own.shape[axis]

    def place(j):
        rows = pl.ds(pl.multiple_of(j * size, size), size)
        return dst.at[rows, :] if axis == 0 else dst.at[:, rows]

    pltpu.make_async_copy(own, place(z), sems.at[0]).start()
    for s in (1, 2, 3):
        j = lax.rem(z - s + 4, 4)

        @pl.when(z >= s)
        def _():
            pltpu.make_async_copy(rest[s - 1], place(j), sems.at[s]).start()

        @pl.when(z < s)
        def _():
            pltpu.make_async_copy(rest[3 + 3 - s], place(j), sems.at[s]).start()


def wait_pieces(pieces, dst, sems, axis):
    size = pieces[0].shape[axis]
    for s in range(4):
        rows = pl.ds(s * size, size)
        view = dst.at[rows, :] if axis == 0 else dst.at[:, rows]
        pltpu.make_async_copy(pieces[0], view, sems.at[s]).wait()


def qkv_kernel(layer, pieces_n, with_q, with_x, rows, *refs):
    z_ref, gain_ref, cos_ref, sin_ref = refs[:4]
    pieces = refs[4:4 + pieces_n]
    wq, wk, wv = refs[4 + pieces_n:7 + pieces_n]
    outs = refs[7 + pieces_n:]
    n_out = 1 + int(with_q) + int(with_x)
    kv_out, rest = outs[0], list(outs[1:n_out])
    q_out = rest.pop(0) if with_q else None
    x_out = rest.pop(0) if with_x else None
    x_vm, h_vm, w_vm, p_sems, w_sems, o_sem = outs[n_out:]
    if pieces_n == 1:
        pltpu.make_async_copy(pieces[0], x_vm, p_sems.at[0]).start()
    else:
        start_pieces(z_ref[0], pieces, x_vm, p_sems, 0)
    sources = (wk, wv, wq) if with_q else (wk, wv)
    copies = [pltpu.make_async_copy(w.at[layer], w_vm.at[i], w_sems.at[i]) for i, w in enumerate(sources)]
    for c in copies:
        c.start()
    if pieces_n == 1:
        pltpu.make_async_copy(pieces[0], x_vm, p_sems.at[0]).wait()
    else:
        wait_pieces(pieces, x_vm, p_sems, 0)
    if with_x:
        x_copy = pltpu.make_async_copy(x_vm, x_out, o_sem)
        x_copy.start()
    gain = gain_ref[...]

    def norm_step(i, carry):
        sl = pl.ds(pl.multiple_of(i * 64, 64), 64)
        h_vm[sl, :] = norm_rows(x_vm[sl, :], gain)
        return carry

    lax.fori_loop(0, rows // 64, norm_step, 0)
    copies[0].wait()
    copies[1].wait()
    heads = [(0, i) for i in range(5)] + [(1, i) for i in range(5)]
    if with_q:
        heads += [(2, i) for i in range(5)]
    waited = False
    for first in range(0, len(heads), 2):
        pair = heads[first:first + 2]
        if any(which == 2 for which, _ in pair) and not waited:
            copies[2].wait()
            waited = True
        weight = jnp.concatenate([w_vm[which, i] for which, i in pair], axis=1) if len(pair) == 2 else w_vm[pair[0]]
        full = jnp.dot(h_vm[...], weight, preferred_element_type=jnp.float32)
        for place, (which, i) in enumerate(pair):
            part = full[:, place * HD:(place + 1) * HD]
            if which != 1:
                part = part * cos_ref[...] + pltpu.roll(part, HD // 2, 1) * sin_ref[...]
            part = part.astype(jnp.bfloat16)
            if which == 2:
                q_out[:, i * HD:(i + 1) * HD] = part
            else:
                kv_out[:, (which * 5 + i) * HD:(which * 5 + i + 1) * HD] = part
    if with_x:
        x_copy.wait()


def qkv(layer, z, gain, cos, sin, pieces, wq, wk, wv, with_q, with_x):
    rows = cos.shape[0]
    dim = pieces[0].shape[1]
    out_shape = [jax.ShapeDtypeStruct((rows, 10 * HD), jnp.bfloat16)]
    out_specs = [VMEM]
    if with_q:
        out_shape.append(jax.ShapeDtypeStruct((rows, 5 * HD), jnp.bfloat16))
        out_specs.append(VMEM)
    if with_x:
        out_shape.append(jax.ShapeDtypeStruct((rows, dim), jnp.bfloat16))
        out_specs.append(ANY)
    n_w = 3 if with_q else 2
    return pl.pallas_call(
        functools.partial(qkv_kernel, layer, len(pieces), with_q, with_x, rows),
        out_shape=out_shape,
        in_specs=[SMEM, VMEM, VMEM, VMEM] + [ANY] * (len(pieces) + 3),
        out_specs=out_specs,
        scratch_shapes=[
            pltpu.VMEM((rows, dim), jnp.bfloat16),
            pltpu.VMEM((rows, dim), jnp.bfloat16),
            pltpu.VMEM((n_w, 5, dim, HD), jnp.bfloat16),
            pltpu.SemaphoreType.DMA((4,)),
            pltpu.SemaphoreType.DMA((3,)),
            pltpu.SemaphoreType.DMA,
        ],
        compiler_params=params(),
        cost_estimate=cost(2 * rows * dim * 5 * HD * n_w, 2 * (rows * dim * 2 + n_w * 5 * dim * HD)),
        name=f"qkv{layer}",
    )(z, gain, cos, sin, *pieces, wq, wk, wv)


def attn_kernel(mode, n_own, scale, *refs):
    r_ref, q_ref = refs[:2]
    n_blk = 4 + n_own
    ks = refs[2:2 + n_blk]
    vs = refs[2 + n_blk:2 + 2 * n_blk]
    o_ref = refs[2 + 2 * n_blk]
    s_vm, mx_vm, l_vm, acc_vm = refs[3 + 2 * n_blk:]
    r = r_ref[0]
    rows = q_ref.shape[0]
    width = ks[0].shape[0]
    if mode == "prompt":
        plan = [(m, "causal" if m == 0 else "if") for m in range(4)]
        order = [0, 1, 2, 3]
    else:
        order = list(range(n_blk))
        plan = [(b, "causal" if b == n_blk - 1 else "full") for b in order]
    coef = scale * LOG2E
    mx_vm[...] = jnp.full(mx_vm.shape, -jnp.inf, jnp.float32)
    l_vm[...] = jnp.zeros(l_vm.shape, jnp.float32)
    acc_vm[...] = jnp.zeros(acc_vm.shape, jnp.float32)

    def scores(b, causal):
        s = lax.dot_general(q_ref[...], ks[b][...], (((1,), (1,)), ((), ())), preferred_element_type=jnp.float32)
        if causal:
            row = lax.broadcasted_iota(jnp.int32, s.shape, 0)
            col = lax.broadcasted_iota(jnp.int32, s.shape, 1)
            s = jnp.where(row >= col, s, -jnp.inf)
        s_vm[:, b * width:(b + 1) * width] = s
        top = mx_vm[...]
        for t in range(width // HD):
            top = jnp.maximum(top, s[:, t * HD:(t + 1) * HD])
        mx_vm[...] = top

    def gather_values(b, m):
        s = s_vm[:, b * width:(b + 1) * width]
        p = jnp.exp2((s - m) * coef)
        total = l_vm[...]
        for t in range(width // HD):
            total = total + p[:, t * HD:(t + 1) * HD]
        l_vm[...] = total
        acc_vm[...] += jnp.dot(p.astype(jnp.bfloat16), vs[b][...], preferred_element_type=jnp.float32)

    for b, kind in plan:
        if kind == "if":
            pl.when((r ^ b) < r)(functools.partial(scores, b, False))
        else:
            scores(b, kind == "causal")
    m = jnp.max(mx_vm[...], axis=1, keepdims=True)
    for b, kind in plan:
        if kind == "if":
            pl.when((r ^ b) < r)(functools.partial(gather_values, b, m))
        else:
            gather_values(b, m)
    o_ref[...] = (acc_vm[...] / jnp.sum(l_vm[...], axis=1, keepdims=True)).astype(jnp.bfloat16)


def attend(mode, r, q, blocks, scale):
    rows = q.shape[0]
    width = blocks[0].shape[0]
    n_own = len(blocks) - 4
    k_spec = pl.BlockSpec((width, HD), lambda h: (0, h))
    v_spec = pl.BlockSpec((width, HD), lambda h: (0, 5 + h))
    seen = len(blocks) * width
    return pl.pallas_call(
        functools.partial(attn_kernel, mode, n_own, scale),
        out_shape=jax.ShapeDtypeStruct((rows, 5 * HD), jnp.bfloat16),
        grid=(5,),
        in_specs=[SMEM, pl.BlockSpec((rows, HD), lambda h: (0, h))] + [k_spec] * len(blocks) + [v_spec] * len(blocks),
        out_specs=pl.BlockSpec((rows, HD), lambda h: (0, h)),
        scratch_shapes=[
            pltpu.VMEM((rows, seen), jnp.float32),
            pltpu.VMEM((rows, HD), jnp.float32),
            pltpu.VMEM((rows, HD), jnp.float32),
            pltpu.VMEM((rows, HD), jnp.float32),
        ],
        compiler_params=params(),
        cost_estimate=cost(8 * rows * seen * HD * 5, 4 * rows * 5 * HD + 4 * seen * 5 * HD, rows * seen * 5),
        name=f"attn_{mode}{n_own}",
    )(r, q, *blocks, *blocks)


def out_kernel(n_w, z_ref, gain_ref, x_ref, *refs):
    pieces, w_ref = refs[:7], refs[7]
    x1_ref, u_ref = refs[8:10]
    o_vm, w_vm, acc_vm, p_sems, w_sems = refs[10:]
    depth = w_vm.shape[1]
    start_pieces(z_ref[0], pieces, o_vm, p_sems, 1)
    copies = [
        pltpu.make_async_copy(w_ref.at[pl.ds(i * depth, depth), :], w_vm.at[i], w_sems.at[i]) for i in range(n_w)
    ]
    for c in copies:
        c.start()
    wait_pieces(pieces, o_vm, p_sems, 1)
    for i, c in enumerate(copies):
        c.wait()
        part = jnp.dot(o_vm[:, i * depth:(i + 1) * depth], w_vm[i], preferred_element_type=jnp.float32)
        if i == 0:
            acc_vm[...] = part
        else:
            acc_vm[...] += part
    gain = gain_ref[...]

    def finish(i, carry):
        sl = pl.ds(pl.multiple_of(i * 64, 64), 64)
        x1 = (x_ref[sl, :].astype(jnp.float32) + acc_vm[sl, :]).astype(jnp.bfloat16)
        x1_ref[sl, :] = x1
        u_ref[sl, :] = norm_rows(x1, gain)
        return carry

    lax.fori_loop(0, acc_vm.shape[0] // 64, finish, 0)


def out_proj(layer, z, gain, x, pieces, w_full):
    rows, dim = x.shape
    n_w = 5
    return pl.pallas_call(
        functools.partial(out_kernel, n_w),
        out_shape=[jax.ShapeDtypeStruct((rows, dim), jnp.bfloat16)] * 2,
        in_specs=[SMEM, VMEM, VMEM] + [ANY] * 8,
        out_specs=[VMEM, VMEM],
        scratch_shapes=[
            pltpu.VMEM((rows, dim), jnp.bfloat16),
            pltpu.VMEM((n_w, dim // n_w, dim), jnp.bfloat16),
            pltpu.VMEM((rows, dim), jnp.float32),
            pltpu.SemaphoreType.DMA((4,)),
            pltpu.SemaphoreType.DMA((n_w,)),
        ],
        compiler_params=params(),
        cost_estimate=cost(2 * rows * dim * dim, 2 * dim * dim + 8 * rows * dim),
        name=f"out{layer}",
    )(z, gain, x, *pieces, w_full)


def head_kernel(n_steps, half, z_ref, gain_ref, tgt_ref, *refs):
    pieces = refs[:7]
    w_ref = refs[7]
    m_ref, l_ref, p_ref = refs[8:11]
    x_vm, h_vm, a_vm, b_vm, mx_vm, sum_vm, pick_vm, p_sems = refs[11:]
    step = pl.program_id(0)
    rows = x_vm.shape[0]

    @pl.when(step == 0)
    def _():
        start_pieces(z_ref[0], pieces, x_vm, p_sems, 0)
        wait_pieces(pieces, x_vm, p_sems, 0)
        gain = gain_ref[...]

        def norm_step(i, carry):
            sl = pl.ds(pl.multiple_of(i * 64, 64), 64)
            h_vm[sl, :] = norm_rows(x_vm[sl, :], gain)
            return carry

        lax.fori_loop(0, rows // 64, norm_step, 0)
        b_vm[...] = jnp.full(b_vm.shape, NEG, jnp.float32)
        mx_vm[...] = jnp.full(mx_vm.shape, NEG, jnp.float32)
        sum_vm[...] = jnp.zeros(sum_vm.shape, jnp.float32)
        pick_vm[...] = jnp.zeros(pick_vm.shape, jnp.float32)

    def fold(src, first, lo, n):
        old = mx_vm[lo:lo + n, :]
        tiles = [src[lo:lo + n, t * HD:(t + 1) * HD] for t in range(half // HD)]
        top = old
        for tile in tiles:
            top = jnp.maximum(top, tile)
        total = sum_vm[lo:lo + n, :] * jnp.exp(old - top)
        pick = pick_vm[lo:lo + n, :]
        want = tgt_ref[lo:lo + n, :] - first
        lane = lax.broadcasted_iota(jnp.int32, (n, HD), 1)
        off = want - lane
        for t, tile in enumerate(tiles):
            total = total + jnp.exp(tile - top)
            pick = pick + jnp.where(off == t * HD, tile, 0.0)
        mx_vm[lo:lo + n, :] = top
        sum_vm[lo:lo + n, :] = total
        pick_vm[lo:lo + n, :] = pick

    def phase(dst, col, src, first):
        n_sub = half // 256
        n = rows // n_sub
        for sub in range(n_sub):
            lo = sub * 256
            dst[:, lo:lo + 256] = jnp.dot(
                h_vm[...], w_ref[:, col + lo:col + lo + 256], preferred_element_type=jnp.float32
            )
            for part in range(n // 32):
                fold(src, first, sub * n + part * 32, 32)

    base = step * 2 * half
    phase(a_vm, 0, b_vm, jnp.where(step == 0, 1 << 30, base - half))
    phase(b_vm, half, a_vm, base)

    @pl.when(step == n_steps - 1)
    def _():
        for part in range(rows // 32):
            fold(b_vm, base + half, part * 32, 32)
        top = jnp.max(mx_vm[...], axis=1, keepdims=True)
        total = jnp.sum(sum_vm[...] * jnp.exp(mx_vm[...] - top), axis=1, keepdims=True)
        pick = jnp.sum(pick_vm[...], axis=1, keepdims=True)
        m_ref[...] = jnp.broadcast_to(top, m_ref.shape)
        l_ref[...] = jnp.broadcast_to(total, l_ref.shape)
        p_ref[...] = jnp.broadcast_to(pick, p_ref.shape)


def head(z, gain, tgt, pieces, w_vocab):
    rows = tgt.shape[0]
    dim, vocab = w_vocab.shape
    half = 1024
    n_steps = vocab // (2 * half)
    full = lambda shape: pl.BlockSpec(shape, lambda i: (0, 0))
    stats = jax.ShapeDtypeStruct((rows, HD), jnp.float32)
    m, l, p = pl.pallas_call(
        functools.partial(head_kernel, n_steps, half),
        out_shape=[stats] * 3,
        grid=(n_steps,),
        in_specs=[SMEM, full((1, dim)), full((rows, 1))] + [ANY] * 7 + [pl.BlockSpec((dim, 2 * half), lambda i: (0, i))],
        out_specs=[full((rows, HD))] * 3,
        scratch_shapes=[
            pltpu.VMEM((rows, dim), jnp.bfloat16),
            pltpu.VMEM((rows, dim), jnp.bfloat16),
            pltpu.VMEM((rows, half), jnp.float32),
            pltpu.VMEM((rows, half), jnp.float32),
            pltpu.VMEM((rows, HD), jnp.float32),
            pltpu.VMEM((rows, HD), jnp.float32),
            pltpu.VMEM((rows, HD), jnp.float32),
            pltpu.SemaphoreType.DMA((4,)),
        ],
        compiler_params=params(),
        cost_estimate=cost(2 * rows * dim * vocab, 2 * dim * vocab, rows * vocab),
        name="head",
    )(z, gain, tgt, *pieces, w_vocab)
    return jnp.stack([m[:, 0], l[:, 0], p[:, 0]])


def gather_pieces(own):
    right, left = [own], [own]
    for s in (1, 2, 3):
        right.append(lax.ppermute(right[-1], 'model', [(i, i + 1) for i in range(s - 1, 3)]))
        left.append(lax.ppermute(left[-1], 'model', [(i, i - 1) for i in range(1, 5 - s)]))
    return (own, *right[1:], *left[1:])


def scatter_sum(part, z):
    from_left = from_right = None
    for t in (1, 2, 3):
        go_right = lax.dynamic_index_in_dim(part, jnp.clip(4 - t + z, 0, 3), 0, keepdims=False)
        go_left = lax.dynamic_index_in_dim(part, jnp.clip(z + t - 4, 0, 3), 0, keepdims=False)
        if t > 1:
            go_right = go_right + from_left
            go_left = go_left + from_right
        from_left = lax.ppermute(go_right, 'model', [(i, i + 1) for i in range(t)])
        from_right = lax.ppermute(go_left, 'model', [(3 - i, 2 - i) for i in range(t)])
    own = lax.dynamic_index_in_dim(part, z, 0, keepdims=False)
    return own + (from_left + from_right)


def solution(mesh):
    row_axes = ('prompts', 'resp')
    head_spec = P(None, None, 'model', None)
    in_specs = (P(row_axes, None), P(row_axes, None, None), P(row_axes, None), P(row_axes), P(None, None), head_spec, head_spec, head_spec, P(None, 'model', None, None), P(None, None), P(None, None, 'model'), P(None, None, 'model'), P(None, 'model', None), P(None), P(None, 'model'))
    groups = mesh.shape['resp']
    spread = groups * mesh.shape['prompts']

    def device_step(x_prompt, x_resp, targets, resp_lens, attn_gain, w_query, w_key, w_value, w_out, mlp_gain, w_gate, w_up, w_down, final_gain, w_vocab):
        chunk = x_prompt.shape[0]
        dim = x_prompt.shape[1]
        resp_len = x_resp.shape[1]
        prompt_len = chunk * groups
        num_layers = w_query.shape[0]
        local = w_out.shape[1] * HD
        z = lax.axis_index('model')
        r = lax.axis_index('resp')
        place = lax.axis_index('prompts') * groups + r
        z_arr = z.astype(jnp.int32).reshape(1)
        r_arr = r.astype(jnp.int32).reshape(1)
        scale = HD ** -0.5

        heads_first = lambda w: jnp.transpose(w, (0, 2, 1, 3))
        wq, wk, wv = heads_first(w_query), heads_first(w_key), heads_first(w_value)

        share = local // spread
        w_out_full = []
        for l in range(num_layers):
            mine = lax.dynamic_slice_in_dim(w_out[l].reshape(local, dim), place * share, share, 0)
            w_out_full.append(lax.all_gather(mine, ('model', 'prompts', 'resp'), axis=0, tiled=True))

        tok_pos = jnp.concatenate([r * chunk + jnp.arange(chunk), prompt_len + jnp.arange(resp_len)])
        half = HD // 2
        frequency = ROPE_BASE ** (-jnp.arange(half, dtype=jnp.float32) / half)
        angles = tok_pos.astype(jnp.float32)[:, None] * frequency
        cos, sin = jnp.cos(angles), jnp.sin(angles)
        cos = jnp.concatenate([cos, cos], axis=1)
        sin = jnp.concatenate([-sin, sin], axis=1)

        n_resp = resp_len // chunk
        n_chunks = 1 + n_resp
        cut = lambda a, c: lax.slice_in_dim(a, c * chunk, (c + 1) * chunk, axis=0)
        pieces = [(x_prompt,)] + [(cut(x_resp[0], c),) for c in range(n_resp)]
        swap = lambda a, bit: lax.ppermute(a, 'resp', [(i, i ^ bit) for i in range(groups)])

        for l in range(num_layers):
            last = l == num_layers - 1
            gain = attn_gain[l][None]
            kvs, qs, xs = [], [], []
            for c in range(n_chunks):
                with_q = not (last and c == 0)
                with_x = len(pieces[c]) > 1 and with_q
                got = qkv(l, z_arr, gain, cut(cos, c), cut(sin, c), pieces[c], wq, wk, wv, with_q, with_x)
                kvs.append(got[0])
                qs.append(got[1] if with_q else None)
                xs.append(got[2] if with_x else pieces[c][0])
            kv2 = swap(kvs[0], 2)
            kv1 = swap(kvs[0], 1)
            kv3 = swap(kv2, 1)
            shared = [kvs[0], kv1, kv2, kv3]
            nxt = [None] * n_chunks
            for c in range(1 if last else 0, n_chunks):
                mode = "prompt" if c == 0 else "resp"
                mixed = attend(mode, r_arr, qs[c], shared + kvs[1:c + 1], scale)
                x1, u = out_proj(l, z_arr, mlp_gain[l][None], xs[c], gather_pieces(mixed), w_out_full[l])
                gate = jnp.dot(u, w_gate[l], preferred_element_type=jnp.float32)
                up_proj = jnp.dot(u, w_up[l], preferred_element_type=jnp.float32)
                inner = (jax.nn.silu(gate) * up_proj).astype(jnp.bfloat16)
                part = jnp.dot(inner, w_down[l], preferred_element_type=jnp.float32)
                summed = scatter_sum(part.reshape(4, chunk // 4, dim), z)
                x_own = lax.dynamic_index_in_dim(x1.reshape(4, chunk // 4, dim), z, 0, keepdims=False)
                x_own = (x_own.astype(jnp.float32) + summed).astype(jnp.bfloat16)
                nxt[c] = gather_pieces(x_own)
            pieces = nxt

        vocab_local = w_vocab.shape[1]
        stats = []
        for c in range(1, n_chunks):
            tgt = cut(targets[0], c - 1)[:, None] - z * vocab_local
            stats.append(head(z_arr, final_gain[None], tgt, pieces[c], w_vocab))
        stats = lax.all_gather(jnp.concatenate(stats, axis=1), 'model', axis=0)
        row_max = jnp.max(stats[:, 0], axis=0)
        exp_total = jnp.sum(stats[:, 1] * jnp.exp(stats[:, 0] - row_max), axis=0)
        picked = jnp.sum(stats[:, 2], axis=0)
        log_probs = picked - row_max - jnp.log(exp_total)
        log_probs = jnp.where(jnp.arange(resp_len) < resp_lens[0], log_probs, 0.0)
        return log_probs[None, :]

    return jax.shard_map(device_step, mesh=mesh, in_specs=in_specs, out_specs=P(row_axes, None), check_vma=False)
```

```python
import functools

import jax
import jax.numpy as jnp
from jax import lax
from jax.experimental import pallas as pl
from jax.experimental.pallas import tpu as pltpu
from jax.sharding import PartitionSpec as P

EPS = 1e-6
ROPE_BASE = 10000.0
LOG2E = 1.4426950408889634
HD = 128
NEG = -1e30
ANY = pl.BlockSpec(memory_space=pl.ANY)
SMEM = pl.BlockSpec(memory_space=pltpu.SMEM)
VMEM = pl.BlockSpec(memory_space=pltpu.VMEM)
VLIMIT = 60 * 1024 * 1024


def params(**kw):
    return pltpu.CompilerParams(vmem_limit_bytes=VLIMIT, **kw)


def cost(flops, nbytes, trans=0):
    return pl.CostEstimate(flops=int(flops), bytes_accessed=int(nbytes), transcendentals=int(trans))


def norm_rows(x, gain):
    x = x.astype(jnp.float32)
    inv = lax.rsqrt(jnp.mean(x * x, axis=-1, keepdims=True) + EPS)
    return (x * inv * gain).astype(jnp.bfloat16)


def start_pieces(z, pieces, dst, sems, axis):
    own, rest = pieces[0], pieces[1:]
    size = own.shape[axis]

    def place(j):
        rows = pl.ds(pl.multiple_of(j * size, size), size)
        return dst.at[rows, :] if axis == 0 else dst.at[:, rows]

    pltpu.make_async_copy(own, place(z), sems.at[0]).start()
    for s in (1, 2, 3):
        j = lax.rem(z - s + 4, 4)

        @pl.when(z >= s)
        def _():
            pltpu.make_async_copy(rest[s - 1], place(j), sems.at[s]).start()

        @pl.when(z < s)
        def _():
            pltpu.make_async_copy(rest[3 + 3 - s], place(j), sems.at[s]).start()


def wait_pieces(pieces, dst, sems, axis):
    size = pieces[0].shape[axis]
    for s in range(4):
        rows = pl.ds(s * size, size)
        view = dst.at[rows, :] if axis == 0 else dst.at[:, rows]
        pltpu.make_async_copy(pieces[0], view, sems.at[s]).wait()


def qkv_kernel(layer, pieces_n, with_q, with_x, rows, *refs):
    z_ref, gain_ref, cos_ref, sin_ref = refs[:4]
    pieces = refs[4:4 + pieces_n]
    wq, wk, wv = refs[4 + pieces_n:7 + pieces_n]
    outs = refs[7 + pieces_n:]
    n_out = 1 + int(with_q) + int(with_x)
    kv_out, rest = outs[0], list(outs[1:n_out])
    q_out = rest.pop(0) if with_q else None
    x_out = rest.pop(0) if with_x else None
    x_vm, h_vm, w_vm, p_sems, w_sems, o_sem = outs[n_out:]
    if pieces_n == 1:
        pltpu.make_async_copy(pieces[0], x_vm, p_sems.at[0]).start()
    else:
        start_pieces(z_ref[0], pieces, x_vm, p_sems, 0)
    sources = (wk, wv, wq) if with_q else (wk, wv)
    copies = []
    for i, w in enumerate(sources):
        for h in range(5):
            j = i * 5 + h
            copies.append(pltpu.make_async_copy(w.at[layer, h], w_vm.at[:, j * HD:(j + 1) * HD], w_sems.at[j]))
    for c in copies:
        c.start()
    if pieces_n == 1:
        pltpu.make_async_copy(pieces[0], x_vm, p_sems.at[0]).wait()
    else:
        wait_pieces(pieces, x_vm, p_sems, 0)
    if with_x:
        x_copy = pltpu.make_async_copy(x_vm, x_out, o_sem)
        x_copy.start()
    gain = gain_ref[...]

    def norm_step(i, carry):
        sl = pl.ds(pl.multiple_of(i * 64, 64), 64)
        h_vm[sl, :] = norm_rows(x_vm[sl, :], gain)
        return carry

    lax.fori_loop(0, rows // 64, norm_step, 0)
    total = len(copies)
    for first in range(0, total, 2):
        pair = range(first, min(first + 2, total))
        for j in pair:
            copies[j].wait()
        full = jnp.dot(h_vm[...], w_vm[:, first * HD:(pair[-1] + 1) * HD], preferred_element_type=jnp.float32)
        for place, j in enumerate(pair):
            part = full[:, place * HD:(place + 1) * HD]
            if j // 5 != 1:
                part = part * cos_ref[...] + pltpu.roll(part, HD // 2, 1) * sin_ref[...]
            part = part.astype(jnp.bfloat16)
            if j >= 10:
                q_out[:, (j - 10) * HD:(j - 9) * HD] = part
            else:
                kv_out[:, j * HD:(j + 1) * HD] = part
    if with_x:
        x_copy.wait()


def qkv(layer, z, gain, cos, sin, pieces, wq, wk, wv, with_q, with_x):
    rows = cos.shape[0]
    dim = pieces[0].shape[1]
    out_shape = [jax.ShapeDtypeStruct((rows, 10 * HD), jnp.bfloat16)]
    out_specs = [VMEM]
    if with_q:
        out_shape.append(jax.ShapeDtypeStruct((rows, 5 * HD), jnp.bfloat16))
        out_specs.append(VMEM)
    if with_x:
        out_shape.append(jax.ShapeDtypeStruct((rows, dim), jnp.bfloat16))
        out_specs.append(ANY)
    n_w = 3 if with_q else 2
    return pl.pallas_call(
        functools.partial(qkv_kernel, layer, len(pieces), with_q, with_x, rows),
        out_shape=out_shape,
        in_specs=[SMEM, VMEM, VMEM, VMEM] + [ANY] * (len(pieces) + 3),
        out_specs=out_specs,
        scratch_shapes=[
            pltpu.VMEM((rows, dim), jnp.bfloat16),
            pltpu.VMEM((rows, dim), jnp.bfloat16),
            pltpu.VMEM((dim, n_w * 5 * HD), jnp.bfloat16),
            pltpu.SemaphoreType.DMA((4,)),
            pltpu.SemaphoreType.DMA((15,)),
            pltpu.SemaphoreType.DMA,
        ],
        compiler_params=params(),
        cost_estimate=cost(2 * rows * dim * 5 * HD * n_w, 2 * (rows * dim * 2 + n_w * 5 * dim * HD)),
        name=f"qkv{layer}",
    )(z, gain, cos, sin, *pieces, wq, wk, wv)


def attn_kernel(mode, n_own, scale, *refs):
    r_ref, q_ref = refs[:2]
    n_blk = 4 + n_own
    ks = refs[2:2 + n_blk]
    vs = refs[2 + n_blk:2 + 2 * n_blk]
    o_ref = refs[2 + 2 * n_blk]
    s_vm, mx_vm, l_vm, acc_vm = refs[3 + 2 * n_blk:]
    r = r_ref[0]
    rows = q_ref.shape[0]
    width = ks[0].shape[0]
    if mode == "prompt":
        plan = [(m, "causal" if m == 0 else "if") for m in range(4)]
        order = [0, 1, 2, 3]
    else:
        order = list(range(n_blk))
        plan = [(b, "causal" if b == n_blk - 1 else "full") for b in order]
    coef = scale * LOG2E
    mx_vm[...] = jnp.full(mx_vm.shape, -jnp.inf, jnp.float32)
    l_vm[...] = jnp.zeros(l_vm.shape, jnp.float32)
    acc_vm[...] = jnp.zeros(acc_vm.shape, jnp.float32)

    def scores(b, causal):
        s = lax.dot_general(q_ref[...], ks[b][...], (((1,), (1,)), ((), ())), preferred_element_type=jnp.float32)
        if causal:
            row = lax.broadcasted_iota(jnp.int32, s.shape, 0)
            col = lax.broadcasted_iota(jnp.int32, s.shape, 1)
            s = jnp.where(row >= col, s, -jnp.inf)
        s_vm[:, b * width:(b + 1) * width] = s
        top = mx_vm[...]
        for t in range(width // HD):
            top = jnp.maximum(top, s[:, t * HD:(t + 1) * HD])
        mx_vm[...] = top

    def gather_values(b, m):
        s = s_vm[:, b * width:(b + 1) * width]
        p = jnp.exp2((s - m) * coef)
        total = l_vm[...]
        for t in range(width // HD):
            total = total + p[:, t * HD:(t + 1) * HD]
        l_vm[...] = total
        acc_vm[...] += jnp.dot(p.astype(jnp.bfloat16), vs[b][...], preferred_element_type=jnp.float32)

    for b, kind in plan:
        if kind == "if":
            pl.when((r ^ b) < r)(functools.partial(scores, b, False))
        else:
            scores(b, kind == "causal")
    m = jnp.max(mx_vm[...], axis=1, keepdims=True)
    for b, kind in plan:
        if kind == "if":
            pl.when((r ^ b) < r)(functools.partial(gather_values, b, m))
        else:
            gather_values(b, m)
    o_ref[...] = (acc_vm[...] / jnp.sum(l_vm[...], axis=1, keepdims=True)).astype(jnp.bfloat16)


def attend(mode, r, q, blocks, scale):
    rows = q.shape[0]
    width = blocks[0].shape[0]
    n_own = len(blocks) - 4
    k_spec = pl.BlockSpec((width, HD), lambda h: (0, h))
    v_spec = pl.BlockSpec((width, HD), lambda h: (0, 5 + h))
    seen = len(blocks) * width
    return pl.pallas_call(
        functools.partial(attn_kernel, mode, n_own, scale),
        out_shape=jax.ShapeDtypeStruct((rows, 5 * HD), jnp.bfloat16),
        grid=(5,),
        in_specs=[SMEM, pl.BlockSpec((rows, HD), lambda h: (0, h))] + [k_spec] * len(blocks) + [v_spec] * len(blocks),
        out_specs=pl.BlockSpec((rows, HD), lambda h: (0, h)),
        scratch_shapes=[
            pltpu.VMEM((rows, seen), jnp.float32),
            pltpu.VMEM((rows, HD), jnp.float32),
            pltpu.VMEM((rows, HD), jnp.float32),
            pltpu.VMEM((rows, HD), jnp.float32),
        ],
        compiler_params=params(),
        cost_estimate=cost(8 * rows * seen * HD * 5, 4 * rows * 5 * HD + 4 * seen * 5 * HD, rows * seen * 5),
        name=f"attn_{mode}{n_own}",
    )(r, q, *blocks, *blocks)


def tail_kernel(layer, z_ref, gain_ref, x_ref, *refs):
    pieces, wo_ref, wg_ref, wu_ref, wd_ref = refs[:7], *refs[7:11]
    x1_ref, part_ref, right_ref, left_ref = refs[11:15]
    o_vm, wo_vm, wg_vm, wu_vm, wd_vm, acc_vm, u_vm, in_vm, p_sems, o_sems, g_sems, d_sems, s_sems = refs[15:]
    rows, dim = x_ref.shape
    hidden = wg_vm.shape[0]
    start_pieces(z_ref[0], pieces, o_vm, p_sems, 1)
    n_sub, _, heads, tall = wo_ref.shape[:4]
    half = dim // 2

    def load_wo(which):
        def body(i, carry):
            n, h = i // heads, i % heads
            for p in range(n_sub):
                dst = pl.ds(pl.multiple_of(i * HD + p * tall, tall), tall)
                cols = pl.ds(which * half, half)
                pltpu.make_async_copy(wo_ref.at[p, n, h, :, cols], wo_vm.at[dst, cols], o_sems.at[which]).start()
            return carry

        lax.fori_loop(0, dim // HD, body, 0)

    load_wo(0)
    load_wo(1)
    blocks = [(lo, min(256, hidden - lo)) for lo in range(0, hidden, 256)]
    g_copies = []
    for i, (lo, n) in enumerate(blocks):
        for k, (src, dst) in enumerate(((wg_ref, wg_vm), (wu_ref, wu_vm))):
            c = pltpu.make_async_copy(src.at[layer, lo:lo + n, :], dst.at[lo:lo + n, :], g_sems.at[k, i])
            c.start()
            g_copies.append(c)
    n_d = d_sems.shape[0]
    wide = dim // n_d
    d_copies = []
    for i in range(n_d):
        c = pltpu.make_async_copy(
            wd_ref.at[layer, :, i * wide:(i + 1) * wide], wd_vm.at[:, i * wide:(i + 1) * wide], d_sems.at[i]
        )
        c.start()
        d_copies.append(c)
    wait_pieces(pieces, o_vm, p_sems, 1)
    for which in range(2):
        cols = wo_vm.at[:, which * half:(which + 1) * half]
        pltpu.make_async_copy(cols, cols, o_sems.at[which]).wait()
        for lo in range(which * half, (which + 1) * half, 256):
            acc_vm[:, lo:lo + 256] = jnp.dot(o_vm[...], wo_vm[:, lo:lo + 256], preferred_element_type=jnp.float32)
    gain = gain_ref[...]

    def finish(i, carry):
        sl = pl.ds(pl.multiple_of(i * 64, 64), 64)
        x1 = (x_ref[sl, :].astype(jnp.float32) + acc_vm[sl, :]).astype(jnp.bfloat16)
        x1_ref[sl, :] = x1
        u_vm[sl, :] = norm_rows(x1, gain)
        return carry

    lax.fori_loop(0, rows // 64, finish, 0)
    nt = (((1,), (1,)), ((), ()))
    for i, (lo, n) in enumerate(blocks):
        g_copies[2 * i].wait()
        g_copies[2 * i + 1].wait()
        gate = lax.dot_general(u_vm[...], wg_vm[lo:lo + n, :], nt, preferred_element_type=jnp.float32)
        up = lax.dot_general(u_vm[...], wu_vm[lo:lo + n, :], nt, preferred_element_type=jnp.float32)
        in_vm[:, lo:lo + n] = (jax.nn.silu(gate) * up).astype(jnp.bfloat16)
    for i in range(n_d):
        d_copies[i].wait()
        for lo in range(i * wide, (i + 1) * wide, 256):
            acc_vm[:, lo:lo + 256] = jnp.dot(in_vm[...], wd_vm[:, lo:lo + 256], preferred_element_type=jnp.float32)
    quarter = rows // 4
    outs = [(acc_vm.at[k * quarter:(k + 1) * quarter, :], part_ref.at[k]) for k in range(4)]
    outs += [(acc_vm.at[3 * quarter:, :], right_ref), (acc_vm.at[:quarter, :], left_ref)]
    s_copies = [pltpu.make_async_copy(src, dst, s_sems.at[k]) for k, (src, dst) in enumerate(outs)]
    for c in s_copies:
        c.start()
    for c in s_copies:
        c.wait()


def tail(layer, z, gain, x, pieces, w_out, w_gate, w_up, w_down):
    rows, dim = x.shape
    hidden = w_gate.shape[1]
    quarter = jax.ShapeDtypeStruct((rows // 4, dim), jnp.float32)
    n_blocks = -(-hidden // 256)
    return pl.pallas_call(
        functools.partial(tail_kernel, layer),
        out_shape=[
            jax.ShapeDtypeStruct((rows, dim), jnp.bfloat16),
            jax.ShapeDtypeStruct((4, rows // 4, dim), jnp.float32),
            quarter,
            quarter,
        ],
        in_specs=[SMEM, VMEM, VMEM] + [ANY] * 11,
        out_specs=[VMEM, ANY, ANY, ANY],
        scratch_shapes=[
            pltpu.VMEM((rows, dim), jnp.bfloat16),
            pltpu.VMEM((dim, dim), jnp.bfloat16),
            pltpu.VMEM((hidden, dim), jnp.bfloat16),
            pltpu.VMEM((hidden, dim), jnp.bfloat16),
            pltpu.VMEM((hidden, dim), jnp.bfloat16),
            pltpu.VMEM((rows, dim), jnp.float32),
            pltpu.VMEM((rows, dim), jnp.bfloat16),
            pltpu.VMEM((rows, hidden), jnp.bfloat16),
            pltpu.SemaphoreType.DMA((4,)),
            pltpu.SemaphoreType.DMA((2,)),
            pltpu.SemaphoreType.DMA((2, n_blocks)),
            pltpu.SemaphoreType.DMA((5,)),
            pltpu.SemaphoreType.DMA((6,)),
        ],
        compiler_params=params(),
        cost_estimate=cost(2 * rows * dim * (dim + 3 * hidden), 2 * dim * (dim + 3 * hidden) + 16 * rows * dim),
        name=f"tail{layer}",
    )(z, gain, x, *pieces, w_out, w_gate, w_up, w_down)


def head_kernel(n_steps, half, z_ref, gain_ref, tgt_ref, *refs):
    pieces = refs[:7]
    w_ref = refs[7]
    m_ref, l_ref, p_ref = refs[8:11]
    x_vm, h_vm, a_vm, b_vm, mx_vm, sum_vm, pick_vm, p_sems = refs[11:]
    step = pl.program_id(0)
    rows = x_vm.shape[0]

    @pl.when(step == 0)
    def _():
        start_pieces(z_ref[0], pieces, x_vm, p_sems, 0)
        wait_pieces(pieces, x_vm, p_sems, 0)
        gain = gain_ref[...]

        def norm_step(i, carry):
            sl = pl.ds(pl.multiple_of(i * 64, 64), 64)
            h_vm[sl, :] = norm_rows(x_vm[sl, :], gain)
            return carry

        lax.fori_loop(0, rows // 64, norm_step, 0)
        b_vm[...] = jnp.full(b_vm.shape, NEG, jnp.float32)
        mx_vm[...] = jnp.full(mx_vm.shape, NEG, jnp.float32)
        sum_vm[...] = jnp.zeros(sum_vm.shape, jnp.float32)
        pick_vm[...] = jnp.zeros(pick_vm.shape, jnp.float32)

    def fold(src, first, lo, n):
        old = mx_vm[lo:lo + n, :]
        tiles = [src[lo:lo + n, t * HD:(t + 1) * HD] for t in range(half // HD)]
        top = old
        for tile in tiles:
            top = jnp.maximum(top, tile)
        total = sum_vm[lo:lo + n, :] * jnp.exp(old - top)
        pick = pick_vm[lo:lo + n, :]
        want = tgt_ref[lo:lo + n, :] - first
        lane = lax.broadcasted_iota(jnp.int32, (n, HD), 1)
        off = want - lane
        for t, tile in enumerate(tiles):
            total = total + jnp.exp(tile - top)
            pick = pick + jnp.where(off == t * HD, tile, 0.0)
        mx_vm[lo:lo + n, :] = top
        sum_vm[lo:lo + n, :] = total
        pick_vm[lo:lo + n, :] = pick

    def phase(dst, col, src, first):
        n_sub = half // 256
        n = rows // n_sub
        for sub in range(n_sub):
            lo = sub * 256
            dst[:, lo:lo + 256] = jnp.dot(
                h_vm[...], w_ref[:, col + lo:col + lo + 256], preferred_element_type=jnp.float32
            )
            for part in range(n // 32):
                fold(src, first, sub * n + part * 32, 32)

    base = step * 2 * half
    phase(a_vm, 0, b_vm, jnp.where(step == 0, 1 << 30, base - half))
    phase(b_vm, half, a_vm, base)

    @pl.when(step == n_steps - 1)
    def _():
        for part in range(rows // 32):
            fold(b_vm, base + half, part * 32, 32)
        top = jnp.max(mx_vm[...], axis=1, keepdims=True)
        total = jnp.sum(sum_vm[...] * jnp.exp(mx_vm[...] - top), axis=1, keepdims=True)
        pick = jnp.sum(pick_vm[...], axis=1, keepdims=True)
        m_ref[...] = jnp.broadcast_to(top, m_ref.shape)
        l_ref[...] = jnp.broadcast_to(total, l_ref.shape)
        p_ref[...] = jnp.broadcast_to(pick, p_ref.shape)


def head(z, gain, tgt, pieces, w_vocab):
    rows = tgt.shape[0]
    dim, vocab = w_vocab.shape
    half = 1024
    n_steps = vocab // (2 * half)
    full = lambda shape: pl.BlockSpec(shape, lambda i: (0, 0))
    stats = jax.ShapeDtypeStruct((rows, HD), jnp.float32)
    m, l, p = pl.pallas_call(
        functools.partial(head_kernel, n_steps, half),
        out_shape=[stats] * 3,
        grid=(n_steps,),
        in_specs=[SMEM, full((1, dim)), full((rows, 1))] + [ANY] * 7 + [pl.BlockSpec((dim, 2 * half), lambda i: (0, i))],
        out_specs=[full((rows, HD))] * 3,
        scratch_shapes=[
            pltpu.VMEM((rows, dim), jnp.bfloat16),
            pltpu.VMEM((rows, dim), jnp.bfloat16),
            pltpu.VMEM((rows, half), jnp.float32),
            pltpu.VMEM((rows, half), jnp.float32),
            pltpu.VMEM((rows, HD), jnp.float32),
            pltpu.VMEM((rows, HD), jnp.float32),
            pltpu.VMEM((rows, HD), jnp.float32),
            pltpu.SemaphoreType.DMA((4,)),
        ],
        compiler_params=params(),
        cost_estimate=cost(2 * rows * dim * vocab, 2 * dim * vocab, rows * vocab),
        name="head",
    )(z, gain, tgt, *pieces, w_vocab)
    return jnp.stack([m[:, 0], l[:, 0], p[:, 0]])


def gather_pieces(own):
    right, left = [own], [own]
    for s in (1, 2, 3):
        right.append(lax.ppermute(right[-1], 'model', [(i, i + 1) for i in range(s - 1, 3)]))
        left.append(lax.ppermute(left[-1], 'model', [(i, i - 1) for i in range(1, 5 - s)]))
    return (own, *right[1:], *left[1:])


def scatter_sum(part, first_right, first_left, z):
    from_left = from_right = None
    for t in (1, 2, 3):
        if t == 1:
            go_right, go_left = first_right, first_left
        else:
            go_right = lax.dynamic_index_in_dim(part, jnp.clip(4 - t + z, 0, 3), 0, keepdims=False) + from_left
            go_left = lax.dynamic_index_in_dim(part, jnp.clip(z + t - 4, 0, 3), 0, keepdims=False) + from_right
        from_left = lax.ppermute(go_right, 'model', [(i, i + 1) for i in range(t)])
        from_right = lax.ppermute(go_left, 'model', [(3 - i, 2 - i) for i in range(t)])
    own = lax.dynamic_index_in_dim(part, z, 0, keepdims=False)
    return own + (from_left + from_right)


def solution(mesh):
    row_axes = ('prompts', 'resp')
    head_spec = P(None, None, 'model', None)
    in_specs = (P(row_axes, None), P(row_axes, None, None), P(row_axes, None), P(row_axes), P(None, None), head_spec, head_spec, head_spec, P(None, 'model', None, None), P(None, None), P(None, None, 'model'), P(None, None, 'model'), P(None, 'model', None), P(None), P(None, 'model'))
    groups = mesh.shape['resp']
    spread = groups * mesh.shape['prompts']

    def device_step(x_prompt, x_resp, targets, resp_lens, attn_gain, w_query, w_key, w_value, w_out, mlp_gain, w_gate, w_up, w_down, final_gain, w_vocab):
        chunk = x_prompt.shape[0]
        dim = x_prompt.shape[1]
        resp_len = x_resp.shape[1]
        prompt_len = chunk * groups
        num_layers = w_query.shape[0]
        z = lax.axis_index('model')
        r = lax.axis_index('resp')
        place = lax.axis_index('prompts') * groups + r
        z_arr = z.astype(jnp.int32).reshape(1)
        r_arr = r.astype(jnp.int32).reshape(1)
        scale = HD ** -0.5

        heads_first = lambda w: jnp.transpose(w, (0, 2, 1, 3))
        wq, wk, wv = heads_first(w_query), heads_first(w_key), heads_first(w_value)

        wg_t, wu_t = jnp.transpose(w_gate, (0, 2, 1)), jnp.transpose(w_up, (0, 2, 1))

        tall = HD // spread
        w_out_full = []
        for l in range(num_layers):
            mine = lax.dynamic_slice_in_dim(w_out[l], place * tall, tall, 1)
            line = lax.all_gather(mine, 'model', axis=0)
            w_out_full.append(lax.all_gather(line, row_axes, axis=0))

        tok_pos = jnp.concatenate([r * chunk + jnp.arange(chunk), prompt_len + jnp.arange(resp_len)])
        half = HD // 2
        frequency = ROPE_BASE ** (-jnp.arange(half, dtype=jnp.float32) / half)
        angles = tok_pos.astype(jnp.float32)[:, None] * frequency
        cos, sin = jnp.cos(angles), jnp.sin(angles)
        cos = jnp.concatenate([cos, cos], axis=1)
        sin = jnp.concatenate([-sin, sin], axis=1)

        n_resp = resp_len // chunk
        n_chunks = 1 + n_resp
        cut = lambda a, c: lax.slice_in_dim(a, c * chunk, (c + 1) * chunk, axis=0)
        pieces = [(x_prompt,)] + [(cut(x_resp[0], c),) for c in range(n_resp)]
        swap = lambda a, bit: lax.ppermute(a, 'resp', [(i, i ^ bit) for i in range(groups)])

        for l in range(num_layers):
            last = l == num_layers - 1
            gain = attn_gain[l][None]
            kvs, qs, xs = [], [], []
            for c in range(n_chunks):
                with_q = not (last and c == 0)
                with_x = len(pieces[c]) > 1 and with_q
                got = qkv(l, z_arr, gain, cut(cos, c), cut(sin, c), pieces[c], wq, wk, wv, with_q, with_x)
                kvs.append(got[0])
                qs.append(got[1] if with_q else None)
                xs.append(got[2] if with_x else pieces[c][0])
            kv2 = swap(kvs[0], 2)
            kv1 = swap(kvs[0], 1)
            kv3 = swap(kv2, 1)
            shared = [kvs[0], kv1, kv2, kv3]
            nxt = [None] * n_chunks
            for c in range(1 if last else 0, n_chunks):
                mode = "prompt" if c == 0 else "resp"
                mixed = attend(mode, r_arr, qs[c], shared + kvs[1:c + 1], scale)
                x1, part, right, left = tail(l, z_arr, mlp_gain[l][None], xs[c], gather_pieces(mixed), w_out_full[l], wg_t, wu_t, w_down)
                summed = scatter_sum(part, right, left, z)
                x_own = lax.dynamic_index_in_dim(x1.reshape(4, chunk // 4, dim), z, 0, keepdims=False)
                x_own = (x_own.astype(jnp.float32) + summed).astype(jnp.bfloat16)
                nxt[c] = gather_pieces(x_own)
            pieces = nxt

        vocab_local = w_vocab.shape[1]
        stats = []
        for c in range(1, n_chunks):
            tgt = cut(targets[0], c - 1)[:, None] - z * vocab_local
            stats.append(head(z_arr, final_gain[None], tgt, pieces[c], w_vocab))
        stats = lax.all_gather(jnp.concatenate(stats, axis=1), 'model', axis=0)
        row_max = jnp.max(stats[:, 0], axis=0)
        exp_total = jnp.sum(stats[:, 1] * jnp.exp(stats[:, 0] - row_max), axis=0)
        picked = jnp.sum(stats[:, 2], axis=0)
        log_probs = picked - row_max - jnp.log(exp_total)
        log_probs = jnp.where(jnp.arange(resp_len) < resp_lens[0], log_probs, 0.0)
        return log_probs[None, :]

    return jax.shard_map(device_step, mesh=mesh, in_specs=in_specs, out_specs=P(row_axes, None), check_vma=False)
```

```python
import functools

import jax
import jax.numpy as jnp
from jax import lax
from jax.experimental import pallas as pl
from jax.experimental.pallas import tpu as pltpu
from jax.sharding import PartitionSpec as P

EPS = 1e-6
ROPE_BASE = 10000.0
LOG2E = 1.4426950408889634
HD = 128
NH = 5
NEG = -1e30
BF, F32 = jnp.bfloat16, jnp.float32
ANY = pl.BlockSpec(memory_space=pl.ANY)
VMEM = pl.BlockSpec(memory_space=pltpu.VMEM)
DMA = pltpu.SemaphoreType.DMA
MESH = pl.DeviceIdType.MESH
NT = (((1,), (1,)), ((), ()))


PLAN = (
    "z0000Q00/k0000z0001Q02/z0002Q01/k0001z0003x0000k0002A00/o000",
    "0A01/x0001o0001o0100A02/x0002o0002z1000o0101o0200x0003o0003T",
    "00/s0000z1001s0010o0102o0201z1002s0001s0011o0103T01/s0002s00",
    "12z1003x1000s0100o0202s0110s0101x1001s0003g0000s0013g0010s01",
    "11o0203T02/g0001g0011x1002s0102s0112s0200g0002x1003s0210g001",
    "2s0103g0100s0201s0113g0003g0110g0013Q10/k1000g0101s0211s0202",
    "g0111g0102s0212s0203k1001g0112g0200k1002g0103s0213g0113g0210",
    "Q11/g0201g0211A11/g0202g0212o1100g0203g0213Q12/o1101A12/o110",
    "2o1103o1200T11/s1100s1110o1201o1202s1101s1111o1203T12/s1102s",
    "1112s1200s1210s1201s1103g1100s1211s1113g1110g1101s1202g1111s",
    "1212g1102s1203g1112g1200s1213g1103g1210g1113H01/g1201g1211g1",
    "202g1212g1203H12/g1213H22/",
)
GROUPS = ((0, 5),)


def read_plan():
    text = "".join(PLAN)
    names = {"Q": "qkv", "A": "attn", "T": "tail", "H": "head", "k": "kv", "z": "wz", "x": "wx", "o": "ago", "s": "rs", "g": "agx"}
    plan, at, hooks, where = [], 0, None, 0
    while at < len(text):
        ch = text[at]
        at += 1
        if ch == "-":
            where += 1
        elif ch == "/":
            hooks = None
        elif ch.isupper():
            hooks, where = {}, -1
            plan.append((names[ch], int(text[at]), int(text[at + 1]), hooks))
            at += 2
        else:
            step = (names[ch],) + tuple(int(d) for d in text[at:at + 4])
            at += 4
            if hooks is None:
                plan.append(step)
            else:
                hooks.setdefault(where, []).append(step)
    return plan


def norm_rows(x, gain):
    x = x.astype(F32)
    inv = lax.rsqrt(jnp.mean(x * x, axis=-1, keepdims=True) + EPS)
    return (x * inv * gain).astype(BF)


def program(sizes, *refs):
    chunk, dim, hidden, vocab, scale = sizes
    half = chunk // 2
    unit = half // 4
    (xp, xr, tgt, again, mgain, fgain, cos, sin, wq, wk, wv, w_out, wg, wu, wd, wvoc) = refs[:16]
    (kvb, kvr, qb, og, og_last, pt, x1b, rr, rl, sr, sl, xg, wf, st_m, st_l, st_p) = refs[16:32]
    (va, vb, vc, vd, xs, lsem, ago_s, ago_r, agx_s, agx_r, rs_s, rs_r, kv_s, kv_r, wz_s, wz_r, wx_s, wx_r) = refs[32:]
    n_piece = 8
    piece = w_out.shape[1] // n_piece
    local = w_out.shape[1]

    z = lax.axis_index('model')
    r = lax.axis_index('resp')
    px = lax.axis_index('prompts')
    y, core = lax.div(r, 2), lax.rem(r, 2)
    r_core, r_y, r_yc = y * 2 + (1 - core), (1 - y) * 2 + core, (1 - y) * 2 + (1 - core)
    others = (r, r_core, r_y, r_yc)
    nx = 1 - px
    ending = []
    free = None

    def remote(src, dst, sems, at, dev):
        return pltpu.make_async_remote_copy(
            src, dst, sems[0].at[at], sems[1].at[at], device_id=dev, device_id_type=MESH)

    def when(cond, body):
        if cond is free:
            body()
        else:
            pl.when(cond)(body)

    def send(cond, *args):
        copy = lambda: remote(*args)
        when(cond, (lambda: copy().wait_send()) if ending else (lambda: copy().start()))

    def recv(cond, ref, *args):
        if not ending:
            when(cond, lambda: remote(ref, ref, *args).wait_recv())

    right, left = {'model': z + 1}, {'model': z - 1}
    to_y, to_core, to_x = {'resp': r_y}, {'resp': r_core}, {'prompts': nx}


    def gather(k, block, sems, at, own=None):
        sides = ((z - k, 0, right), (3 - z - k, 1, left))
        for room, side, to in sides:
            j = lax.rem(z + 4 + (2 * side - 1) * k, 4)
            src = own if own is not None and k == 0 else block(j)
            if k:
                recv(room >= 0, src, sems, at + (k - 1, side), to)
            if k < 3:
                ahead = z <= 2 if side == 0 else z >= 1
                send((room >= 0) & ahead, src, block(j), sems, at + (k, side), to)

    def heads_out(l, c, g, j):
        return (og_last if g else og).at[l, c, j]

    def step_ago(l, c, g, k):
        gather(k, lambda j: heads_out(l, c, g, j), (ago_s, ago_r), (l, c, g))

    def rows_at(g, j):
        return pl.ds(pl.multiple_of(g * half + j * unit, 16), unit)

    def step_agx(l, c, g, k):
        gather(k, lambda j: xg.at[l, c, rows_at(g, j)], (agx_s, agx_r), (l, c, g))

    def load(*pairs):
        copies = [pltpu.make_async_copy(s, d, lsem.at[i]) for i, (s, d) in enumerate(pairs)]
        for cp in copies:
            cp.start()
        for cp in copies:
            cp.wait()

    def add_rows(dst, *srcs):
        def body(i, carry):
            sl_ = pl.ds(pl.multiple_of(i * 16, 16), 16)
            total = srcs[0][sl_, :]
            for s in srcs[1:]:
                total = total + s[sl_, :]
            dst[sl_, :] = total
            return carry

        lax.fori_loop(0, unit // 16, body, 0)

    def step_rs(l, c, g, k):
        part, r_in, l_in, r_out, l_out = (lambda j: pt.at[l, c, rows_at(g, j)]), rr.at[l, c, g], rl.at[l, c, g], sr.at[l, c, g], sl.at[l, c, g]
        sems, at = (rs_s, rs_r), (l, c, g)
        if k < 3:
            send(z == 0, part(3 - k), r_in.at[k], sems, at + (k, 0), right)
            send(z == 3, part(k), l_in.at[k], sems, at + (k, 1), left)
        if k == 1:
            for cond, side, far, src, out, to in ((z == 1, 0, 3, r_in, r_out, right), (z == 2, 1, 0, l_in, l_out, left)):
                recv(cond, src.at[0], sems, at + (0, side), to)
                if not ending:
                    @pl.when(cond)
                    def _():
                        load((part(far), va), (src.at[0], vb))
                        add_rows(va, va, vb)
                        load((va, out.at[0]))
                send(cond, out.at[0], src.at[1], sems, at + (1, side), to)
        elif k == 2:
            mid = (z >= 1) & (z <= 2)
            sides = ((0, r_in, r_out, right), (1, l_in, l_out, left))
            for side, src, out, to in sides:
                recv(mid, src.at[1], sems, at + (1, side), to)
            if not ending:
                @pl.when(mid)
                def _():
                    load((part(z + 1), va), (r_in.at[1], vb), (part(z - 1), vc), (l_in.at[1], vd))
                    add_rows(va, va, vb)
                    add_rows(vc, vc, vd)
                    load((va, r_out.at[1]), (vc, l_out.at[1]))
            for side, src, out, to in sides:
                send(mid, out.at[1], src.at[2], sems, at + (2, side), to)
        elif k == 3 and not ending:
            ends = ((2, z >= 1, r_in.at[2], vb, right), (3, z <= 2, l_in.at[2], vc, left))
            for idx, cond, src, dst, to in ends:
                recv(cond, src, sems, at + (2, idx - 2), to)
            copies = [pltpu.make_async_copy(part(z), va, lsem.at[0]), pltpu.make_async_copy(x1b.at[l, c, g], xs, lsem.at[1])]
            for cp in copies:
                cp.start()
            for idx, cond, src, dst, _ in ends:
                @pl.when(cond)
                def _():
                    one = pltpu.make_async_copy(src, dst, lsem.at[idx])
                    one.start()
                    one.wait()

                @pl.when(jnp.logical_not(cond))
                def _():
                    dst[...] = jnp.zeros(dst.shape, F32)
            for cp in copies:
                cp.wait()

            def body(i, carry):
                s_ = pl.ds(pl.multiple_of(i * 16, 16), 16)
                total = va[s_, :] + (vb[s_, :] + vc[s_, :])
                xs[s_, :] = (xs[s_, :].astype(F32) + total).astype(BF)
                return carry

            lax.fori_loop(0, unit // 16, body, 0)
            load((xs, xg.at[l, c, rows_at(g, z)]))

    def step_kv(l, c, g, k):
        slots, sems = [kvr.at[l, i] for i in range(3)], (kv_s, kv_r)
        if k == 0:
            send(free, kvb.at[l, 0], slots[1], sems, (l, 1), to_y)
            send(free, kvb.at[l, 0], slots[0], sems, (l, 0), to_core)
        elif k == 1:
            recv(free, slots[1], sems, (l, 1), to_y)
            send(free, slots[1], slots[2], sems, (l, 2), to_core)
        else:
            recv(free, slots[0], sems, (l, 0), to_core)
            recv(free, slots[2], sems, (l, 2), to_core)

    def rows_of(j, rr_, xx):
        return pl.ds(pl.multiple_of(j * local + (xx * 4 + rr_) * piece, 16), piece)

    def step_wz(l, c, g, k):
        own = w_out.at[l, pl.ds(pl.multiple_of((px * 4 + r) * piece, 16), piece), :]
        gather(k, lambda j: wf.at[l, rows_of(j, r, px), :], (wz_s, wz_r), (l,), own)

    def step_wx(l, c, g, k):
        for s in range(3):
            j = lax.rem(z + 1 + s, 4)

            def push(i, place, to):
                at = wf.at[l, rows_of(j, *place), :]
                send(free, at, at, (wx_s, wx_r), (l, i, s), to)

            def pull(i, place, to):
                recv(free, wf.at[l, rows_of(j, *place), :], (wx_s, wx_r), (l, i, s), to)

            here, over_y, over_x, over_xy = (r, px), (r_y, px), (r, nx), (r_y, nx)
            if k == 0:
                push(0, here, to_y)
                push(1, here, to_x)
            elif k == 1:
                pull(0, over_y, to_y)
                push(2, over_y, to_x)
            elif k == 2:
                pull(1, over_x, to_x)
                pull(2, over_xy, to_x)
                for i, place in enumerate((here, over_y, over_x, over_xy)):
                    push(3 + i, place, to_core)
            else:
                for i, place in enumerate(((r_core, px), (r_yc, px), (r_core, nx), (r_yc, nx))):
                    pull(3 + i, place, to_core)

    steps = {"ago": step_ago, "agx": step_agx, "rs": step_rs, "kv": step_kv, "wz": step_wz, "wx": step_wx}

    def emit(item):
        steps[item[0]](*item[1:])

    def pre(hooks):
        for item in hooks.get(-1, []):
            emit(item)

    def loop(n, body, hooks, base):
        begin = 0
        for i in range(n):
            if hooks.get(base + i) or i == n - 1:
                lax.fori_loop(begin, i + 1, lambda k, carry: (body(k), carry)[1], 0)
                begin = i + 1
                for item in hooks.get(base + i, []):
                    emit(item)


    def load_x(l, c, x_vm, sem, first=0):
        rows = pl.ds(first, x_vm.shape[0])
        if l:
            src = xg.at[l - 1, c, rows]
        elif c:
            src = xr.at[0, pl.ds((c - 1) * chunk, chunk)]
        else:
            src = xp
        copy = pltpu.make_async_copy(src, x_vm, sem.at[0])
        copy.start()
        return copy

    def norm_all(src, dst, gain):
        rows = src.shape[0]

        def body(i, carry):
            s_ = pl.ds(pl.multiple_of(i * 32, 32), 32)
            dst[s_, :] = norm_rows(src[s_, :], gain)
            return carry

        lax.fori_loop(0, rows // 32, body, 0)

    def task_qkv(l, c, hooks):
        with_q = not (l == 1 and c == 0)
        kinds = (wk, wq, wv) if with_q else (wk, wv)
        n_w = NH * len(kinds)

        def scoped(x_vm, w_vm, o_vm, cs_vm, x_sems, w_sems, o_sems, c_sems):
            c_copies = [pltpu.make_async_copy(src.at[c], cs_vm.at[i], c_sems.at[i]) for i, src in enumerate((cos, sin))]
            w_copies = [pltpu.make_async_copy(w.at[l], w_vm.at[NH * i:NH * (i + 1)], w_sems.at[i]) for i, w in enumerate(kinds)]
            for cp in c_copies + w_copies:
                cp.start()
            pre(hooks)
            load_x(l, c, x_vm, x_sems).wait()
            norm_all(x_vm, x_vm, again[l:l + 1, :])
            for cp in c_copies + w_copies:
                cp.wait()
            cs, sn = cs_vm[0], cs_vm[1]

            def rope(part):
                return part * cs + pltpu.roll(part, HD // 2, 1) * sn

            def pair(i, ropes):
                both = jnp.concatenate([w_vm[i], w_vm[i + 1]], axis=1)
                full = jnp.dot(x_vm[...], both, preferred_element_type=F32)
                for n, with_rope in enumerate(ropes):
                    part = full[:, n * HD:(n + 1) * HD]
                    o_vm[i + n] = (rope(part) if with_rope else part).astype(BF)

            n_rope = n_w - NH

            loop(n_rope // 2, lambda i: pair(2 * i, (True, True)), hooks, 0)
            first = n_rope
            if n_rope % 2:
                pair(n_rope - 1, (True, False))
                first = n_rope + 1

            loop(2, lambda i: pair(first + 2 * i, (False, False)), hooks, 5)
            if first + 4 < n_w:
                o_vm[n_w - 1] = jnp.dot(x_vm[...], w_vm[n_w - 1], preferred_element_type=F32).astype(BF)
            outs = [(o_vm.at[0:NH], kvb.at[l, c, 0:NH]), (o_vm.at[n_w - NH:n_w], kvb.at[l, c, NH:2 * NH])]
            if with_q:
                outs.append((o_vm.at[NH:2 * NH], qb.at[l, c]))
            o_copies = [pltpu.make_async_copy(s, d, o_sems.at[i]) for i, (s, d) in enumerate(outs)]
            for cp in o_copies:
                cp.start()
            for cp in o_copies:
                cp.wait()

        pl.run_scoped(
            scoped, pltpu.VMEM((chunk, dim), BF), pltpu.VMEM((n_w, dim, HD), BF), pltpu.VMEM((n_w, chunk, HD), BF),
            pltpu.VMEM((2, chunk, HD), F32), DMA((1,)), DMA((3,)), DMA((3,)), DMA((2,)),
        )

    def task_attn(l, c, hooks):
        blocks = [kvb.at[l, 0], kvr.at[l, 0], kvr.at[l, 1], kvr.at[l, 2]] + [kvb.at[l, i] for i in range(1, c + 1)]
        n_blk = len(blocks)
        if c == 0:
            plan = [(0, "causal")] + [(m, "if") for m in (1, 2, 3)]
        else:
            plan = [(b, "causal" if b == n_blk - 1 else "full") for b in range(n_blk)]
        coef = scale * LOG2E

        def scoped(q_vm, kv_vm, s_vm, mx_vm, l_vm, acc_vm, o_vm, sems):
            copies = [pltpu.make_async_copy(qb.at[l, c], q_vm, sems.at[n_blk])]
            copies += [pltpu.make_async_copy(src, kv_vm.at[b], sems.at[b]) for b, src in enumerate(blocks)]
            pre(hooks)
            for cp in copies:
                cp.start()
            for cp in copies:
                cp.wait()

            def head_body(h):
                mx_vm[...] = jnp.full(mx_vm.shape, -jnp.inf, F32)
                l_vm[...] = jnp.zeros(l_vm.shape, F32)
                acc_vm[...] = jnp.zeros(acc_vm.shape, F32)

                def scores(b, causal):
                    s = lax.dot_general(q_vm[h], kv_vm[b, h], NT, preferred_element_type=F32)
                    if causal:
                        row = lax.broadcasted_iota(jnp.int32, s.shape, 0)
                        col = lax.broadcasted_iota(jnp.int32, s.shape, 1)
                        s = jnp.where(row >= col, s, -jnp.inf)
                    s_vm[:, b * chunk:(b + 1) * chunk] = s
                    top = mx_vm[...]
                    for t in range(chunk // HD):
                        top = jnp.maximum(top, s[:, t * HD:(t + 1) * HD])
                    mx_vm[...] = top

                def mix(b, m):
                    p = jnp.exp2((s_vm[:, b * chunk:(b + 1) * chunk] - m) * coef)
                    total = l_vm[...]
                    for t in range(chunk // HD):
                        total = total + p[:, t * HD:(t + 1) * HD]
                    l_vm[...] = total
                    acc_vm[...] += jnp.dot(p.astype(BF), kv_vm[b, NH + h], preferred_element_type=F32)

                for b, kind in plan:
                    if kind == "if":
                        pl.when(others[b] < r)(functools.partial(scores, b, False))
                    else:
                        scores(b, kind == "causal")
                m = jnp.max(mx_vm[...], axis=1, keepdims=True)
                for b, kind in plan:
                    if kind == "if":
                        pl.when(others[b] < r)(functools.partial(mix, b, m))
                    else:
                        mix(b, m)
                out = (acc_vm[...] / jnp.sum(l_vm[...], axis=1, keepdims=True)).astype(BF)
                o_vm[:, pl.ds(pl.multiple_of(h * HD, HD), HD)] = out

            for g, (first, end) in enumerate(GROUPS):
                lax.fori_loop(first, end, lambda h, carry: (head_body(h), carry)[1], 0)
                out_copy = pltpu.make_async_copy(o_vm.at[:, first * HD:end * HD], heads_out(l, c, g, z), sems.at[0])
                out_copy.start()
                out_copy.wait()
                for item in hooks.get(end - 1, []):
                    emit(item)

        pl.run_scoped(
            scoped, pltpu.VMEM((NH, chunk, HD), BF), pltpu.VMEM((n_blk, 2 * NH, chunk, HD), BF),
            pltpu.VMEM((chunk, n_blk * chunk), F32), pltpu.VMEM((chunk, HD), F32), pltpu.VMEM((chunk, HD), F32),
            pltpu.VMEM((chunk, HD), F32), pltpu.VMEM((chunk, NH * HD), BF), DMA((n_blk + 1,)),
        )

    def task_tail(l, c, hooks):
        full_blocks, rest = hidden // 256, hidden % 256

        def scoped(o_vm, x_vm, wo_vm, wg_vm, wu_vm, wd_vm, acc_vm, in_vm, o_sems, x_sems, wo_sems, w_sems, p_sems):
            wo_copies = [pltpu.make_async_copy(
                w_out.at[l], wo_vm.at[pl.ds(pl.multiple_of(z * local, 128), local), :], wo_sems.at[0])]
            for s in (1, 2, 3):
                rows = pl.ds(pl.multiple_of(lax.rem(z + s, 4) * local, 128), local)
                wo_copies.append(pltpu.make_async_copy(wf.at[l, rows, :], wo_vm.at[rows, :], wo_sems.at[s]))
            for cp in wo_copies:
                cp.start()
            x_copy = load_x(l, c, x_vm, x_sems)
            w_copies = [pltpu.make_async_copy(s.at[l], d, w_sems.at[i]) for i, (s, d) in enumerate(((wg, wg_vm), (wu, wu_vm), (wd, wd_vm)))]
            for cp in w_copies:
                cp.start()
            pre(hooks)
            o_copies = []
            for j in range(4):
                for g, (first, end) in enumerate(GROUPS):
                    cols = o_vm.at[:, j * local + first * HD:j * local + end * HD]
                    o_copies.append(pltpu.make_async_copy(heads_out(l, c, g, j), cols, o_sems.at[j, g]))
            for cp in o_copies:
                cp.start()
            for cp in wo_copies + o_copies:
                cp.wait()
            wide = dim // 5

            def out_body(i):
                cols = pl.ds(pl.multiple_of(i * wide, 128), wide)
                acc_vm[:, cols] = jnp.dot(o_vm[...], wo_vm[:, cols], preferred_element_type=F32)

            loop(5, out_body, hooks, 0)
            x_copy.wait()
            gain = mgain[l:l + 1, :]

            def finish(i, carry):
                s_ = pl.ds(pl.multiple_of(i * 32, 32), 32)
                x1 = (x_vm[s_, :].astype(F32) + acc_vm[s_, :]).astype(BF)
                x_vm[s_, :] = x1
                o_vm[s_, :] = norm_rows(x1, gain)
                return carry

            lax.fori_loop(0, chunk // 32, finish, 0)
            x1_copies = [
                pltpu.make_async_copy(
                    x_vm.at[pl.ds(pl.multiple_of(g * half + z * unit, 16), unit), :], x1b.at[l, c, g], x_sems.at[g])
                for g in range(2)
            ]
            for cp in x1_copies:
                cp.start()
            w_copies[0].wait()
            w_copies[1].wait()

            def gate_up(rows, cols):
                gate = lax.dot_general(o_vm[...], wg_vm[rows, :], NT, preferred_element_type=F32)
                up = lax.dot_general(o_vm[...], wu_vm[rows, :], NT, preferred_element_type=F32)
                in_vm[:, cols] = (jax.nn.silu(gate) * up).astype(BF)

            def gate_body(i):
                s_ = pl.ds(pl.multiple_of(i * 256, 256), 256)
                gate_up(s_, s_)

            loop(full_blocks, gate_body, hooks, 5)
            if rest:
                s_ = pl.ds(full_blocks * 256, rest)
                gate_up(s_, s_)
            w_copies[2].wait()

            for cp in x1_copies:
                cp.wait()
            for g in range(2):
                top = g * half

                def down_body(i):
                    cols = pl.ds(pl.multiple_of(i * wide, 128), wide)
                    acc_vm[top:top + half, cols] = jnp.dot(in_vm[top:top + half, :], wd_vm[:, cols], preferred_element_type=F32)

                lax.fori_loop(0, 5, lambda i, carry: (down_body(i), carry)[1], 0)
                p_copy = pltpu.make_async_copy(acc_vm.at[top:top + half], pt.at[l, c, pl.ds(top, half)], p_sems.at[g])
                p_copy.start()
                p_copy.wait()
                for item in hooks.get(9 + full_blocks + 5 * g, []):
                    emit(item)

        pl.run_scoped(
            scoped, pltpu.VMEM((chunk, dim), BF), pltpu.VMEM((chunk, dim), BF), pltpu.VMEM((4 * local, dim), BF),
            pltpu.VMEM((hidden, dim), BF), pltpu.VMEM((hidden, dim), BF), pltpu.VMEM((hidden, dim), BF),
            pltpu.VMEM((chunk, dim), F32), pltpu.VMEM((chunk, hidden), BF),
            DMA((4, 2)), DMA((2,)), DMA((4,)), DMA((3,)), DMA((2,)),
        )

    def task_head(mode, c, hooks):
        wide = 1024
        n_steps = vocab // (2 * wide)
        rows = half if mode else chunk
        begin = (mode - 1) * half if mode else 0
        out = c - 1

        def scoped(h_vm, w_vm, a_vm, b_vm, mx_vm, sum_vm, pick_vm, want_vm, x_sems, w_sems):
            def fetch(i, slot):
                cols = pl.ds(pl.multiple_of(i * 2 * wide, 2 * wide), 2 * wide)
                return pltpu.make_async_copy(wvoc.at[:, cols], w_vm.at[slot], w_sems.at[slot])

            fetch(0, 0).start()
            pre(hooks)
            load_x(2, c, h_vm, x_sems, begin).wait()
            norm_all(h_vm, h_vm, fgain[...])
            want_vm[...] = tgt[out, begin:begin + rows, :]
            b_vm[...] = jnp.full(b_vm.shape, NEG, F32)
            mx_vm[...] = jnp.full(mx_vm.shape, NEG, F32)
            sum_vm[...] = jnp.zeros(sum_vm.shape, F32)
            pick_vm[...] = jnp.zeros(pick_vm.shape, F32)

            def fold(src, first, at):
                old = mx_vm[at, :]
                tiles = [src[at, t * HD:(t + 1) * HD] for t in range(wide // HD)]
                top = old
                for tile in tiles:
                    top = jnp.maximum(top, tile)
                total = sum_vm[at, :] * jnp.exp(old - top)
                pick = pick_vm[at, :]
                lane = lax.broadcasted_iota(jnp.int32, old.shape, 1)
                off = want_vm[at, :] - first - lane
                for t, tile in enumerate(tiles):
                    total = total + jnp.exp(tile - top)
                    pick = pick + jnp.where(off == t * HD, tile, 0.0)
                mx_vm[at, :] = top
                sum_vm[at, :] = total
                pick_vm[at, :] = pick

            def folds(src, first, lo, n):
                step = lambda i, carry: (fold(src, first, pl.ds(pl.multiple_of(lo + i * 32, 32), 32)), carry)[1]
                lax.fori_loop(0, n // 32, step, 0)

            def phase(dst, slot, col, src, first):
                n_sub = wide // 256
                n = rows // n_sub
                for sub in range(n_sub):
                    lo = sub * 256
                    dst[:, lo:lo + 256] = jnp.dot(
                        h_vm[...], w_vm[slot, :, col + lo:col + lo + 256], preferred_element_type=F32)
                    folds(src, first, sub * n, n)

            def body(i):
                slot = lax.rem(i, 2)

                @pl.when(i + 1 < n_steps)
                def _():
                    fetch(i + 1, 1 - slot).start()

                fetch(i, slot).wait()
                base = i * 2 * wide
                phase(a_vm, slot, 0, b_vm, jnp.where(i == 0, vocab * 8, base - wide))
                phase(b_vm, slot, wide, a_vm, base)

            loop(n_steps, body, hooks, 0)
            folds(b_vm, vocab - wide, 0, rows)
            top = jnp.max(mx_vm[...], axis=1, keepdims=True)
            total = jnp.sum(sum_vm[...] * jnp.exp(mx_vm[...] - top), axis=1, keepdims=True)
            pick = jnp.sum(pick_vm[...], axis=1, keepdims=True)
            st_m[out, begin:begin + rows, :] = jnp.broadcast_to(top, (rows, HD))
            st_l[out, begin:begin + rows, :] = jnp.broadcast_to(total, (rows, HD))
            st_p[out, begin:begin + rows, :] = jnp.broadcast_to(pick, (rows, HD))

        pl.run_scoped(
            scoped, pltpu.VMEM((rows, dim), BF), pltpu.VMEM((2, dim, 2 * wide), BF),
            pltpu.VMEM((rows, wide), F32), pltpu.VMEM((rows, wide), F32), pltpu.VMEM((rows, HD), F32),
            pltpu.VMEM((rows, HD), F32), pltpu.VMEM((rows, HD), F32), pltpu.VMEM((rows, 1), jnp.int32), DMA((1,)), DMA((2,)),
        )

    tasks = {"qkv": task_qkv, "attn": task_attn, "tail": task_tail, "head": task_head}

    barrier = pltpu.get_barrier_semaphore()

    def greet(dev):
        pl.semaphore_signal(barrier, inc=1, device_id=dev, device_id_type=MESH)

    for dev in (to_core, to_y, to_x):
        greet(dev)
    pl.when(z <= 2)(lambda: greet(right))
    pl.when(z >= 1)(lambda: greet(left))
    pl.semaphore_wait(barrier, 3 + lax.div(z + 2, 3) + lax.div(5 - z, 3))

    plan = read_plan()
    for entry in plan:
        if entry[0] in tasks:
            tasks[entry[0]](*entry[1:])
        else:
            emit(entry)
    ending.append(True)
    for entry in plan:
        for item in (sum(entry[-1].values(), []) if entry[0] in tasks else [entry]):
            emit(item)


def solution(mesh):
    row_axes = ('prompts', 'resp')
    rows, whole, second, third = P(row_axes), P(), P(None, 'model'), P(None, None, 'model')
    in_specs = (rows, rows, rows, rows, whole, third, third, third, second, whole, third, third, second, whole, second)
    groups = mesh.shape['resp']

    def device_step(x_prompt, x_resp, targets, resp_lens, attn_gain, w_query, w_key, w_value, w_out, mlp_gain, w_gate, w_up, w_down, final_gain, w_vocab):
        chunk, dim = x_prompt.shape
        resp_len = x_resp.shape[1]
        prompt_len = chunk * groups
        n_l = w_query.shape[0]
        hidden = w_gate.shape[2]
        vocab = w_vocab.shape[1]
        local = w_out.shape[1] * HD
        z = lax.axis_index('model')
        r = lax.axis_index('resp')
        heads_first = lambda w: jnp.transpose(w, (0, 2, 1, 3))

        tok_pos = jnp.concatenate([r * chunk + jnp.arange(chunk), prompt_len + jnp.arange(resp_len)])
        half = HD // 2
        frequency = ROPE_BASE ** (-jnp.arange(half, dtype=F32) / half)
        angles = tok_pos.astype(F32)[:, None] * frequency
        cos, sin = jnp.cos(angles), jnp.sin(angles)
        n_resp = resp_len // chunk
        n_c = 1 + n_resp
        cos = jnp.concatenate([cos, cos], axis=1).reshape(n_c, chunk, HD)
        sin = jnp.concatenate([-sin, sin], axis=1).reshape(n_c, chunk, HD)
        tgt = (targets[0] - z * vocab).reshape(n_resp, chunk, 1)
        unit = chunk // 8

        sds = jax.ShapeDtypeStruct
        out_shape = [
            sds((n_l, n_c, 2 * NH, chunk, HD), BF), sds((n_l, 3, 2 * NH, chunk, HD), BF), sds((n_l, n_c, NH, chunk, HD), BF),
            sds((n_l, n_c, 4, chunk, 5 * HD), BF), sds((n_l, n_c, 4, chunk, HD), BF), sds((n_l, n_c, chunk, dim), F32), sds((n_l, n_c, 2, unit, dim), BF),
            sds((n_l, n_c, 2, 3, unit, dim), F32), sds((n_l, n_c, 2, 3, unit, dim), F32),
            sds((n_l, n_c, 2, 2, unit, dim), F32), sds((n_l, n_c, 2, 2, unit, dim), F32),
            sds((n_l, n_c, chunk, dim), BF), sds((n_l, 4 * local, dim), BF),
        ] + [sds((n_resp, chunk, HD), F32)] * 3
        gsem = lambda g: DMA((n_l, n_c) + g + (3, 2))
        outs = pl.pallas_call(
            functools.partial(program, (chunk, dim, hidden, vocab, HD ** -0.5)),
            out_shape=out_shape,
            in_specs=[ANY, ANY, VMEM, VMEM, VMEM, VMEM] + [ANY] * 10,
            out_specs=[ANY] * 13 + [VMEM] * 3,
            scratch_shapes=[pltpu.VMEM((unit, dim), F32)] * 4 + [pltpu.VMEM((unit, dim), BF), DMA((4,))] + [gsem((1,))] * 2 + [gsem((2,))] * 4
            + [DMA((n_l, 3))] * 2 + [DMA((n_l, 3, 2))] * 2 + [DMA((n_l, 7, 3))] * 2,
            compiler_params=pltpu.CompilerParams(collective_id=0, has_side_effects=True, vmem_limit_bytes=67043328),
            name="decoder",
        )(x_prompt, x_resp, tgt, attn_gain, mlp_gain, final_gain[None], cos, sin, heads_first(w_query), heads_first(w_key), heads_first(w_value), w_out.reshape(n_l, local, dim), jnp.transpose(w_gate, (0, 2, 1)), jnp.transpose(w_up, (0, 2, 1)), w_down, w_vocab)
        stats = jnp.stack([s[:, :, 0].reshape(resp_len) for s in outs[13:]])
        stats = lax.all_gather(stats, 'model', axis=0)
        row_max = jnp.max(stats[:, 0], axis=0)
        exp_total = jnp.sum(stats[:, 1] * jnp.exp(stats[:, 0] - row_max), axis=0)
        picked = jnp.sum(stats[:, 2], axis=0)
        log_probs = picked - row_max - jnp.log(exp_total)
        log_probs = jnp.where(jnp.arange(resp_len) < resp_lens[0], log_probs, 0.0)
        return log_probs[None, :]

    return jax.shard_map(device_step, mesh=mesh, in_specs=in_specs, out_specs=rows, check_vma=False)
```

```python
import functools

import jax
import jax.numpy as jnp
from jax import lax
from jax.experimental import pallas as pl
from jax.experimental.pallas import tpu as pltpu
from jax.sharding import PartitionSpec as P

EPS = 1e-6
ROPE_BASE = 10000.0
LOG2E = 1.4426950408889634
HD = 128
NH = 5
NEG = -1e30
BF, F32 = jnp.bfloat16, jnp.float32
ANY = pl.BlockSpec(memory_space=pl.ANY)
VMEM = pl.BlockSpec(memory_space=pltpu.VMEM)
DMA = pltpu.SemaphoreType.DMA
MESH = pl.DeviceIdType.MESH
NT = (((1,), (1,)), ((), ()))


PLAN = (
    "z00Q00-------z01/k00Q01-------z02/Q02-------z03x00/k01A00k02",
    "-----o00/A01-----o01o10x01/A02-----o02o20/x02o11x03o03T00---",
    "--o21---z30--------s00o12-----s04/o22s01z31s05o13T01-----s02",
    "o23---s06z32--------s10-----s03/T02-----s07g00g04s11z33x30--",
    "----s14-----g01-----g05s12x31/s15g02g06s20s13x32Q10g10g03s24",
    "g07-------x33/k30s16g11s21s17k31g12g14s25k32s22g13g15s26s23g",
    "20g16s27g24g21Q11g17-------g25/g22A11-----g23g26o40/Q12g27/o",
    "41A12-----o42o50/T11o43--------o51--------s40-----s44o52/T12",
    "o53--------s41---s45-----s50/s42s46s43g40s47g44s51g41s54g45s",
    "52g42g46s55s53g50g43H01g47----g51s56----g52s57g54/H12g53----",
    "g55----g56/H22g57/",
)
GROUPS = ((0, 5),)


def read_plan():
    text = "".join(PLAN)
    names = {"Q": "qkv", "A": "attn", "T": "tail", "H": "head"}
    plan, hooks, where = [], None, 0
    marks = iter(text)
    for mark in marks:
        if mark == "-":
            where += 1
        elif mark == "/":
            hooks = None
        elif mark.isupper():
            hooks, where = {}, -1
            plan.append((names[mark], int(next(marks)), int(next(marks)), hooks))
        else:
            at, k = int(next(marks)), int(next(marks))
            step = (mark, at // 3, at % 3, k // 4, k % 4)
            if hooks is None:
                plan.append(step)
            else:
                hooks.setdefault(where, []).append(step)
    return plan


def norm_rows(x, gain):
    x = x.astype(F32)
    inv = lax.rsqrt(jnp.mean(x * x, axis=-1, keepdims=True) + EPS)
    return (x * inv * gain).astype(BF)


def program(sizes, *refs):
    chunk, dim, hidden, vocab, scale = sizes
    half = chunk // 2
    unit = half // 4
    (xp, xr, tgt, again, mgain, fgain, cos, sin, wq, wk, wv, w_out, wg, wu, wd, wvoc) = refs[:16]
    (kvb, kvr, qb, og, og_last, pt, x1b, rr, rl, sr, sl, xg, wf, st_m, st_l, st_p) = refs[16:32]
    (va, vb, vc, vd, xs, lsem, ago_s, ago_r, agx_s, agx_r, rs_s, rs_r, kv_s, kv_r, wz_s, wz_r, wx_s, wx_r) = refs[32:]
    n_piece = 8
    piece = w_out.shape[1] // n_piece
    local = w_out.shape[1]

    z = lax.axis_index('model')
    r = lax.axis_index('resp')
    px = lax.axis_index('prompts')
    y, core = lax.div(r, 2), lax.rem(r, 2)
    r_core, r_y, r_yc = y * 2 + (1 - core), (1 - y) * 2 + core, (1 - y) * 2 + (1 - core)
    others = (r, r_core, r_y, r_yc)
    nx = 1 - px
    ending = []
    free = None

    def remote(src, dst, sems, at, dev):
        return pltpu.make_async_remote_copy(
            src, dst, sems[0].at[at], sems[1].at[at], device_id=dev, device_id_type=MESH)

    def when(cond, body):
        if cond is free:
            body()
        else:
            pl.when(cond)(body)

    def send(cond, *args):
        copy = lambda: remote(*args)
        when(cond, (lambda: copy().wait_send()) if ending else (lambda: copy().start()))

    def recv(cond, ref, *args):
        if not ending:
            when(cond, lambda: remote(ref, ref, *args).wait_recv())

    right, left = (px, z + 1, r), (px, z - 1, r)
    to_y, to_core, to_x = (px, z, r_y), (px, z, r_core), (nx, z, r)


    def gather(k, block, sems, at, own=None):
        sides = ((z - k, 0, right), (3 - z - k, 1, left))
        for room, side, to in sides:
            j = lax.rem(z + 4 + (2 * side - 1) * k, 4)
            src = own if own is not None and k == 0 else block(j)
            if k:
                recv(room >= 0, src, sems, at + (k - 1, side), to)
            if k < 3:
                ahead = z <= 2 if side == 0 else z >= 1
                send((room >= 0) & ahead, src, block(j), sems, at + (k, side), to)

    def heads_out(l, c, g, j):
        return (og_last if g else og).at[l, c, j]

    def step_ago(l, c, g, k):
        gather(k, lambda j: heads_out(l, c, g, j), (ago_s, ago_r), (l, c, g))

    def rows_at(g, j):
        return pl.ds(pl.multiple_of(g * half + j * unit, 16), unit)

    def step_agx(l, c, g, k):
        gather(k, lambda j: xg.at[l, c, rows_at(g, j)], (agx_s, agx_r), (l, c, g))

    def load(*pairs):
        copies = [pltpu.make_async_copy(s, d, lsem.at[i]) for i, (s, d) in enumerate(pairs)]
        for cp in copies:
            cp.start()
        for cp in copies:
            cp.wait()

    def add_rows(dst, *srcs):
        def body(i, carry):
            sl_ = pl.ds(pl.multiple_of(i * 16, 16), 16)
            total = srcs[0][sl_, :]
            for s in srcs[1:]:
                total = total + s[sl_, :]
            dst[sl_, :] = total
            return carry

        lax.fori_loop(0, unit // 16, body, 0)

    def step_rs(l, c, g, k):
        part, r_in, l_in, r_out, l_out = (lambda j: pt.at[l, c, rows_at(g, j)]), rr.at[l, c, g], rl.at[l, c, g], sr.at[l, c, g], sl.at[l, c, g]
        sems, at = (rs_s, rs_r), (l, c, g)
        if k < 3:
            send(z == 0, part(3 - k), r_in.at[k], sems, at + (k, 0), right)
            send(z == 3, part(k), l_in.at[k], sems, at + (k, 1), left)
        if k == 1:
            for cond, side, far, src, out, to in ((z == 1, 0, 3, r_in, r_out, right), (z == 2, 1, 0, l_in, l_out, left)):
                recv(cond, src.at[0], sems, at + (0, side), to)
                if not ending:
                    @pl.when(cond)
                    def _():
                        load((part(far), va), (src.at[0], vb))
                        add_rows(va, va, vb)
                        load((va, out.at[0]))
                send(cond, out.at[0], src.at[1], sems, at + (1, side), to)
        elif k == 2:
            mid = (z >= 1) & (z <= 2)
            sides = ((0, r_in, r_out, right), (1, l_in, l_out, left))
            for side, src, out, to in sides:
                recv(mid, src.at[1], sems, at + (1, side), to)
            if not ending:
                @pl.when(mid)
                def _():
                    load((part(z + 1), va), (r_in.at[1], vb), (part(z - 1), vc), (l_in.at[1], vd))
                    add_rows(va, va, vb)
                    add_rows(vc, vc, vd)
                    load((va, r_out.at[1]), (vc, l_out.at[1]))
            for side, src, out, to in sides:
                send(mid, out.at[1], src.at[2], sems, at + (2, side), to)
        elif k == 3 and not ending:
            ends = ((2, z >= 1, r_in.at[2], vb, right), (3, z <= 2, l_in.at[2], vc, left))
            for idx, cond, src, dst, to in ends:
                recv(cond, src, sems, at + (2, idx - 2), to)
            copies = [pltpu.make_async_copy(part(z), va, lsem.at[0]), pltpu.make_async_copy(x1b.at[l, c, g], xs, lsem.at[1])]
            for cp in copies:
                cp.start()
            for idx, cond, src, dst, _ in ends:
                @pl.when(cond)
                def _():
                    one = pltpu.make_async_copy(src, dst, lsem.at[idx])
                    one.start()
                    one.wait()

                @pl.when(jnp.logical_not(cond))
                def _():
                    dst[...] = jnp.zeros(dst.shape, F32)
            for cp in copies:
                cp.wait()

            def body(i, carry):
                s_ = pl.ds(pl.multiple_of(i * 16, 16), 16)
                total = va[s_, :] + (vb[s_, :] + vc[s_, :])
                xs[s_, :] = (xs[s_, :].astype(F32) + total).astype(BF)
                return carry

            lax.fori_loop(0, unit // 16, body, 0)
            load((xs, xg.at[l, c, rows_at(g, z)]))

    def step_kv(l, c, g, k):
        slots, sems = [kvr.at[l, i] for i in range(3)], (kv_s, kv_r)
        if k == 0:
            send(free, kvb.at[l, 0], slots[1], sems, (l, 1), to_y)
            send(free, kvb.at[l, 0], slots[0], sems, (l, 0), to_core)
        elif k == 1:
            recv(free, slots[1], sems, (l, 1), to_y)
            send(free, slots[1], slots[2], sems, (l, 2), to_core)
        else:
            recv(free, slots[0], sems, (l, 0), to_core)
            recv(free, slots[2], sems, (l, 2), to_core)

    def rows_of(j, rr_, xx):
        return pl.ds(pl.multiple_of(j * local + (xx * 4 + rr_) * piece, 16), piece)

    def step_wz(l, c, g, k):
        own = w_out.at[l, pl.ds(pl.multiple_of((px * 4 + r) * piece, 16), piece), :]
        gather(k, lambda j: wf.at[l, rows_of(j, r, px), :], (wz_s, wz_r), (l,), own)

    def step_wx(l, c, g, k):
        for s in range(3):
            j = lax.rem(z + 1 + s, 4)

            def push(i, place, to):
                at = wf.at[l, rows_of(j, *place), :]
                send(free, at, at, (wx_s, wx_r), (l, i, s), to)

            def pull(i, place, to):
                recv(free, wf.at[l, rows_of(j, *place), :], (wx_s, wx_r), (l, i, s), to)

            here, over_y, over_x, over_xy = (r, px), (r_y, px), (r, nx), (r_y, nx)
            if k == 0:
                push(0, here, to_y)
                push(1, here, to_x)
            elif k == 1:
                pull(0, over_y, to_y)
                push(2, over_y, to_x)
            elif k == 2:
                pull(1, over_x, to_x)
                pull(2, over_xy, to_x)
                for i, place in enumerate((here, over_y, over_x, over_xy)):
                    push(3 + i, place, to_core)
            else:
                for i, place in enumerate(((r_core, px), (r_yc, px), (r_core, nx), (r_yc, nx))):
                    pull(3 + i, place, to_core)

    steps = {"o": step_ago, "g": step_agx, "s": step_rs, "k": step_kv, "z": step_wz, "x": step_wx}

    def emit(item):
        steps[item[0]](*item[1:])

    def pre(hooks):
        for item in hooks.get(-1, []):
            emit(item)

    def loop(n, body, hooks, base):
        begin = 0
        for i in range(n):
            if hooks.get(base + i) or i == n - 1:
                lax.fori_loop(begin, i + 1, lambda k, carry: (body(k), carry)[1], 0)
                begin = i + 1
                for item in hooks.get(base + i, []):
                    emit(item)

    def steps_of(n, body, hooks, base):
        for i in range(n):
            body(i)
            for item in hooks.get(base + i, []):
                emit(item)


    def load_x(l, c, x_vm, sem, first=0):
        rows = pl.ds(first, x_vm.shape[0])
        if l:
            src = xg.at[l - 1, c, rows]
        elif c:
            src = xr.at[0, pl.ds((c - 1) * chunk, chunk)]
        else:
            src = xp
        copy = pltpu.make_async_copy(src, x_vm, sem.at[0])
        copy.start()
        return copy

    def norm_all(src, dst, gain):
        rows = src.shape[0]

        def body(i, carry):
            s_ = pl.ds(pl.multiple_of(i * 32, 32), 32)
            dst[s_, :] = norm_rows(src[s_, :], gain)
            return carry

        lax.fori_loop(0, rows // 32, body, 0)

    def task_qkv(l, c, hooks):
        with_q = not (l == 1 and c == 0)
        kinds = (wk, wq, wv) if with_q else (wk, wv)
        n_w = NH * len(kinds)

        def scoped(x_vm, w_vm, o_vm, cs_vm, x_sems, w_sems, o_sems, c_sems):
            c_copies = [pltpu.make_async_copy(src.at[c], cs_vm.at[i], c_sems.at[i]) for i, src in enumerate((cos, sin))]
            w_copies = [pltpu.make_async_copy(w.at[l], w_vm.at[NH * i:NH * (i + 1)], w_sems.at[i]) for i, w in enumerate(kinds)]
            for cp in c_copies + w_copies:
                cp.start()
            pre(hooks)
            load_x(l, c, x_vm, x_sems).wait()
            norm_all(x_vm, x_vm, again[l:l + 1, :])
            for cp in c_copies + w_copies:
                cp.wait()
            cs, sn = cs_vm[0], cs_vm[1]

            def rope(part):
                return part * cs + pltpu.roll(part, HD // 2, 1) * sn

            def pair(i, ropes):
                both = jnp.concatenate([w_vm[i], w_vm[i + 1]], axis=1)
                full = jnp.dot(x_vm[...], both, preferred_element_type=F32)
                for n, with_rope in enumerate(ropes):
                    part = full[:, n * HD:(n + 1) * HD]
                    o_vm[i + n] = (rope(part) if with_rope else part).astype(BF)

            n_rope = n_w - NH

            steps_of(n_rope // 2, lambda i: pair(2 * i, (True, True)), hooks, 0)
            first = n_rope
            if n_rope % 2:
                pair(n_rope - 1, (True, False))
                first = n_rope + 1

            steps_of(2, lambda i: pair(first + 2 * i, (False, False)), hooks, 5)
            if first + 4 < n_w:
                o_vm[n_w - 1] = jnp.dot(x_vm[...], w_vm[n_w - 1], preferred_element_type=F32).astype(BF)
            outs = [(o_vm.at[0:NH], kvb.at[l, c, 0:NH]), (o_vm.at[n_w - NH:n_w], kvb.at[l, c, NH:2 * NH])]
            if with_q:
                outs.append((o_vm.at[NH:2 * NH], qb.at[l, c]))
            o_copies = [pltpu.make_async_copy(s, d, o_sems.at[i]) for i, (s, d) in enumerate(outs)]
            for cp in o_copies:
                cp.start()
            for cp in o_copies:
                cp.wait()

        pl.run_scoped(
            scoped, pltpu.VMEM((chunk, dim), BF), pltpu.VMEM((n_w, dim, HD), BF), pltpu.VMEM((n_w, chunk, HD), BF),
            pltpu.VMEM((2, chunk, HD), F32), DMA((1,)), DMA((3,)), DMA((3,)), DMA((2,)),
        )

    def task_attn(l, c, hooks):
        blocks = [kvb.at[l, 0], kvr.at[l, 0], kvr.at[l, 1], kvr.at[l, 2]] + [kvb.at[l, i] for i in range(1, c + 1)]
        n_blk = len(blocks)
        if c == 0:
            plan = [(0, "causal")] + [(m, "if") for m in (1, 2, 3)]
        else:
            plan = [(b, "causal" if b == n_blk - 1 else "full") for b in range(n_blk)]
        coef = scale * LOG2E

        def scoped(q_vm, kv_vm, s_vm, mx_vm, l_vm, acc_vm, o_vm, sems):
            copies = [pltpu.make_async_copy(qb.at[l, c], q_vm, sems.at[n_blk])]
            copies += [pltpu.make_async_copy(src, kv_vm.at[b], sems.at[b]) for b, src in enumerate(blocks)]
            pre(hooks)
            for cp in copies:
                cp.start()
            for cp in copies:
                cp.wait()

            def head_body(h):
                mx_vm[...] = jnp.full(mx_vm.shape, -jnp.inf, F32)
                l_vm[...] = jnp.zeros(l_vm.shape, F32)
                acc_vm[...] = jnp.zeros(acc_vm.shape, F32)

                def scores(b, causal):
                    s = lax.dot_general(q_vm[h], kv_vm[b, h], NT, preferred_element_type=F32)
                    if causal:
                        row = lax.broadcasted_iota(jnp.int32, s.shape, 0)
                        col = lax.broadcasted_iota(jnp.int32, s.shape, 1)
                        s = jnp.where(row >= col, s, -jnp.inf)
                    s_vm[:, b * chunk:(b + 1) * chunk] = s
                    top = mx_vm[...]
                    for t in range(chunk // HD):
                        top = jnp.maximum(top, s[:, t * HD:(t + 1) * HD])
                    mx_vm[...] = top

                def mix(b, m):
                    p = jnp.exp2((s_vm[:, b * chunk:(b + 1) * chunk] - m) * coef)
                    total = l_vm[...]
                    for t in range(chunk // HD):
                        total = total + p[:, t * HD:(t + 1) * HD]
                    l_vm[...] = total
                    acc_vm[...] += jnp.dot(p.astype(BF), kv_vm[b, NH + h], preferred_element_type=F32)

                for b, kind in plan:
                    if kind == "if":
                        pl.when(others[b] < r)(functools.partial(scores, b, False))
                    else:
                        scores(b, kind == "causal")
                m = jnp.max(mx_vm[...], axis=1, keepdims=True)
                for b, kind in plan:
                    if kind == "if":
                        pl.when(others[b] < r)(functools.partial(mix, b, m))
                    else:
                        mix(b, m)
                out = (acc_vm[...] / jnp.sum(l_vm[...], axis=1, keepdims=True)).astype(BF)
                o_vm[:, pl.ds(pl.multiple_of(h * HD, HD), HD)] = out

            for g, (first, end) in enumerate(GROUPS):
                lax.fori_loop(first, end, lambda h, carry: (head_body(h), carry)[1], 0)
                out_copy = pltpu.make_async_copy(o_vm.at[:, first * HD:end * HD], heads_out(l, c, g, z), sems.at[0])
                out_copy.start()
                out_copy.wait()
                for item in hooks.get(end - 1, []):
                    emit(item)

        pl.run_scoped(
            scoped, pltpu.VMEM((NH, chunk, HD), BF), pltpu.VMEM((n_blk, 2 * NH, chunk, HD), BF),
            pltpu.VMEM((chunk, n_blk * chunk), F32), pltpu.VMEM((chunk, HD), F32), pltpu.VMEM((chunk, HD), F32),
            pltpu.VMEM((chunk, HD), F32), pltpu.VMEM((chunk, NH * HD), BF), DMA((n_blk + 1,)),
        )

    def task_tail(l, c, hooks):
        full_blocks, rest = hidden // 256, hidden % 256

        def scoped(o_vm, x_vm, wo_vm, wg_vm, wu_vm, wd_vm, acc_vm, in_vm, o_sems, x_sems, wo_sems, w_sems, p_sems):
            wo_copies = [pltpu.make_async_copy(
                w_out.at[l], wo_vm.at[pl.ds(pl.multiple_of(z * local, 128), local), :], wo_sems.at[0])]
            for s in (1, 2, 3):
                rows = pl.ds(pl.multiple_of(lax.rem(z + s, 4) * local, 128), local)
                wo_copies.append(pltpu.make_async_copy(wf.at[l, rows, :], wo_vm.at[rows, :], wo_sems.at[s]))
            for cp in wo_copies:
                cp.start()
            x_copy = load_x(l, c, x_vm, x_sems)
            w_copies = [pltpu.make_async_copy(s.at[l], d, w_sems.at[i]) for i, (s, d) in enumerate(((wg, wg_vm), (wu, wu_vm), (wd, wd_vm)))]
            for cp in w_copies:
                cp.start()
            pre(hooks)
            o_copies = []
            for j in range(4):
                for g, (first, end) in enumerate(GROUPS):
                    cols = o_vm.at[:, j * local + first * HD:j * local + end * HD]
                    o_copies.append(pltpu.make_async_copy(heads_out(l, c, g, j), cols, o_sems.at[j, g]))
            for cp in o_copies:
                cp.start()
            for cp in wo_copies + o_copies:
                cp.wait()
            wide = dim // 5

            def out_body(i):
                cols = pl.ds(i * wide, wide)
                acc_vm[:, cols] = jnp.dot(o_vm[...], wo_vm[:, cols], preferred_element_type=F32)

            steps_of(5, out_body, hooks, 0)
            x_copy.wait()
            gain = mgain[l:l + 1, :]

            def finish(i, carry):
                s_ = pl.ds(pl.multiple_of(i * 32, 32), 32)
                x1 = (x_vm[s_, :].astype(F32) + acc_vm[s_, :]).astype(BF)
                x_vm[s_, :] = x1
                o_vm[s_, :] = norm_rows(x1, gain)
                return carry

            lax.fori_loop(0, chunk // 32, finish, 0)
            x1_copies = [
                pltpu.make_async_copy(
                    x_vm.at[pl.ds(pl.multiple_of(g * half + z * unit, 16), unit), :], x1b.at[l, c, g], x_sems.at[g])
                for g in range(2)
            ]
            for cp in x1_copies:
                cp.start()
            w_copies[0].wait()
            w_copies[1].wait()

            def gate_up(rows, cols):
                gate = lax.dot_general(o_vm[...], wg_vm[rows, :], NT, preferred_element_type=F32)
                up = lax.dot_general(o_vm[...], wu_vm[rows, :], NT, preferred_element_type=F32)
                in_vm[:, cols] = (jax.nn.silu(gate) * up).astype(BF)

            def gate_body(i):
                s_ = pl.ds(i * 256, 256)
                gate_up(s_, s_)

            steps_of(full_blocks, gate_body, hooks, 5)
            if rest:
                s_ = pl.ds(full_blocks * 256, rest)
                gate_up(s_, s_)
            w_copies[2].wait()

            for cp in x1_copies:
                cp.wait()
            for g in range(2):
                top = g * half

                def down_body(i):
                    cols = pl.ds(i * wide, wide)
                    acc_vm[top:top + half, cols] = jnp.dot(in_vm[top:top + half, :], wd_vm[:, cols], preferred_element_type=F32)

                steps_of(5, down_body, {}, 0)
                p_copy = pltpu.make_async_copy(acc_vm.at[top:top + half], pt.at[l, c, pl.ds(top, half)], p_sems.at[g])
                p_copy.start()
                p_copy.wait()
                for item in hooks.get(9 + full_blocks + 5 * g, []):
                    emit(item)

        pl.run_scoped(
            scoped, pltpu.VMEM((chunk, dim), BF), pltpu.VMEM((chunk, dim), BF), pltpu.VMEM((4 * local, dim), BF),
            pltpu.VMEM((hidden, dim), BF), pltpu.VMEM((hidden, dim), BF), pltpu.VMEM((hidden, dim), BF),
            pltpu.VMEM((chunk, dim), F32), pltpu.VMEM((chunk, hidden), BF),
            DMA((4, 2)), DMA((2,)), DMA((4,)), DMA((3,)), DMA((2,)),
        )

    def task_head(mode, c, hooks):
        wide = 1024
        n_steps = vocab // (2 * wide)
        rows = half if mode else chunk
        begin = (mode - 1) * half if mode else 0
        out = c - 1

        def scoped(h_vm, w_vm, a_vm, b_vm, mx_vm, sum_vm, pick_vm, want_vm, x_sems, w_sems):
            def fetch(i, slot):
                cols = pl.ds(pl.multiple_of(i * 2 * wide, 2 * wide), 2 * wide)
                return pltpu.make_async_copy(wvoc.at[:, cols], w_vm.at[slot], w_sems.at[slot])

            fetch(0, 0).start()
            pre(hooks)
            load_x(2, c, h_vm, x_sems, begin).wait()
            norm_all(h_vm, h_vm, fgain[...])
            want_vm[...] = tgt[out, begin:begin + rows, :]
            b_vm[...] = jnp.full(b_vm.shape, NEG, F32)
            mx_vm[...] = jnp.full(mx_vm.shape, NEG, F32)
            sum_vm[...] = jnp.zeros(sum_vm.shape, F32)
            pick_vm[...] = jnp.zeros(pick_vm.shape, F32)

            def narrow(x, op):
                while x.shape[1] > HD:
                    mid = x.shape[1] // 2
                    x = op(x[:, :mid], x[:, mid:])
                return x

            def fold(src, first, at):
                block, old = src[at, :], mx_vm[at, :]
                top = jnp.maximum(old, narrow(block, jnp.maximum))
                terms = jnp.exp(block - jnp.concatenate([top] * (wide // HD), axis=1))
                hit = want_vm[at, :] - first == lax.broadcasted_iota(jnp.int32, block.shape, 1)
                mx_vm[at, :] = top
                sum_vm[at, :] = sum_vm[at, :] * jnp.exp(old - top) + narrow(terms, jnp.add)
                pick_vm[at, :] += narrow(jnp.where(hit, block, 0.0), jnp.add)

            def folds(src, first, lo, n):
                for i in range(n // 32):
                    fold(src, first, pl.ds(lo + i * 32, 32))

            def phase(dst, slot, col, src, first):
                n_sub = wide // 256
                n = rows // n_sub
                for sub in range(n_sub):
                    lo = sub * 256
                    dst[:, lo:lo + 256] = jnp.dot(
                        h_vm[...], w_vm[slot, :, col + lo:col + lo + 256], preferred_element_type=F32)
                    folds(src, first, sub * n, n)

            def body(i):
                slot = lax.rem(i, 2)

                @pl.when(i + 1 < n_steps)
                def _():
                    fetch(i + 1, 1 - slot).start()

                fetch(i, slot).wait()
                base = i * 2 * wide
                phase(a_vm, slot, 0, b_vm, jnp.where(i == 0, vocab * 8, base - wide))
                phase(b_vm, slot, wide, a_vm, base)

            loop(n_steps, body, hooks, 0)
            last_fold = lambda i, carry: (fold(b_vm, vocab - wide, pl.ds(pl.multiple_of(i * 32, 32), 32)), carry)[1]
            lax.fori_loop(0, rows // 32, last_fold, 0)
            top = jnp.max(mx_vm[...], axis=1, keepdims=True)
            total = jnp.sum(sum_vm[...] * jnp.exp(mx_vm[...] - top), axis=1, keepdims=True)
            pick = jnp.sum(pick_vm[...], axis=1, keepdims=True)
            st_m[out, begin:begin + rows, :] = jnp.broadcast_to(top, (rows, HD))
            st_l[out, begin:begin + rows, :] = jnp.broadcast_to(total, (rows, HD))
            st_p[out, begin:begin + rows, :] = jnp.broadcast_to(pick, (rows, HD))

        pl.run_scoped(
            scoped, pltpu.VMEM((rows, dim), BF), pltpu.VMEM((2, dim, 2 * wide), BF),
            pltpu.VMEM((rows, wide), F32), pltpu.VMEM((rows, wide), F32), pltpu.VMEM((rows, HD), F32),
            pltpu.VMEM((rows, HD), F32), pltpu.VMEM((rows, HD), F32), pltpu.VMEM((rows, 1), jnp.int32), DMA((1,)), DMA((2,)),
        )

    tasks = {"qkv": task_qkv, "attn": task_attn, "tail": task_tail, "head": task_head}

    barrier = pltpu.get_barrier_semaphore()

    def greet(dev):
        pl.semaphore_signal(barrier, inc=1, device_id=dev, device_id_type=MESH)

    for dev in (to_core, to_y, to_x):
        greet(dev)
    pl.when(z <= 2)(lambda: greet(right))
    pl.when(z >= 1)(lambda: greet(left))
    pl.semaphore_wait(barrier, 3 + lax.div(z + 2, 3) + lax.div(5 - z, 3))

    plan = read_plan()
    for entry in plan:
        if entry[0] in tasks:
            tasks[entry[0]](*entry[1:])
        else:
            emit(entry)
    ending.append(True)
    for entry in plan:
        for item in (sum(entry[-1].values(), []) if entry[0] in tasks else [entry]):
            emit(item)


def solution(mesh):
    row_axes = ('prompts', 'resp')
    rows, whole, second, third = P(row_axes), P(), P(None, 'model'), P(None, None, 'model')
    in_specs = (rows, rows, rows, rows, whole, third, third, third, second, whole, third, third, second, whole, second)
    groups = mesh.shape['resp']

    def device_step(x_prompt, x_resp, targets, resp_lens, attn_gain, w_query, w_key, w_value, w_out, mlp_gain, w_gate, w_up, w_down, final_gain, w_vocab):
        chunk, dim = x_prompt.shape
        resp_len = x_resp.shape[1]
        prompt_len = chunk * groups
        n_l = w_query.shape[0]
        hidden = w_gate.shape[2]
        vocab = w_vocab.shape[1]
        local = w_out.shape[1] * HD
        z = lax.axis_index('model')
        r = lax.axis_index('resp')
        heads_first = lambda w: jnp.transpose(w, (0, 2, 1, 3))

        tok_pos = jnp.concatenate([r * chunk + jnp.arange(chunk), prompt_len + jnp.arange(resp_len)])
        half = HD // 2
        frequency = ROPE_BASE ** (-jnp.arange(half, dtype=F32) / half)
        angles = tok_pos.astype(F32)[:, None] * frequency
        cos, sin = jnp.cos(angles), jnp.sin(angles)
        n_resp = resp_len // chunk
        n_c = 1 + n_resp
        cos = jnp.concatenate([cos, cos], axis=1).reshape(n_c, chunk, HD)
        sin = jnp.concatenate([-sin, sin], axis=1).reshape(n_c, chunk, HD)
        tgt = (targets[0] - z * vocab).reshape(n_resp, chunk, 1)
        unit = chunk // 8

        sds = jax.ShapeDtypeStruct
        out_shape = [
            sds((n_l, n_c, 2 * NH, chunk, HD), BF), sds((n_l, 3, 2 * NH, chunk, HD), BF), sds((n_l, n_c, NH, chunk, HD), BF),
            sds((n_l, n_c, 4, chunk, 5 * HD), BF), sds((n_l, n_c, 4, chunk, HD), BF), sds((n_l, n_c, chunk, dim), F32), sds((n_l, n_c, 2, unit, dim), BF),
            sds((n_l, n_c, 2, 3, unit, dim), F32), sds((n_l, n_c, 2, 3, unit, dim), F32),
            sds((n_l, n_c, 2, 2, unit, dim), F32), sds((n_l, n_c, 2, 2, unit, dim), F32),
            sds((n_l, n_c, chunk, dim), BF), sds((n_l, 4 * local, dim), BF),
        ] + [sds((n_resp, chunk, HD), F32)] * 3
        gsem = lambda g: DMA((n_l, n_c) + g + (3, 2))
        outs = pl.pallas_call(
            functools.partial(program, (chunk, dim, hidden, vocab, HD ** -0.5)),
            out_shape=out_shape,
            in_specs=[ANY, ANY, VMEM, VMEM, VMEM, VMEM] + [ANY] * 10,
            out_specs=[ANY] * 13 + [VMEM] * 3,
            scratch_shapes=[pltpu.VMEM((unit, dim), F32)] * 4 + [pltpu.VMEM((unit, dim), BF), DMA((4,))] + [gsem((1,))] * 2 + [gsem((2,))] * 4
            + [DMA((n_l, 3))] * 2 + [DMA((n_l, 3, 2))] * 2 + [DMA((n_l, 7, 3))] * 2,
            compiler_params=pltpu.CompilerParams(collective_id=0, has_side_effects=True, vmem_limit_bytes=67043328),
            name="decoder",
        )(x_prompt, x_resp, tgt, attn_gain, mlp_gain, final_gain[None], cos, sin, heads_first(w_query), heads_first(w_key), heads_first(w_value), w_out.reshape(n_l, local, dim), jnp.transpose(w_gate, (0, 2, 1)), jnp.transpose(w_up, (0, 2, 1)), w_down, w_vocab)
        stats = jnp.stack([s[:, :, 0].reshape(resp_len) for s in outs[13:]])
        stats = lax.all_gather(stats, 'model', axis=0)
        row_max = jnp.max(stats[:, 0], axis=0)
        exp_total = jnp.sum(stats[:, 1] * jnp.exp(stats[:, 0] - row_max), axis=0)
        picked = jnp.sum(stats[:, 2], axis=0)
        log_probs = picked - row_max - jnp.log(exp_total)
        log_probs = jnp.where(jnp.arange(resp_len) < resp_lens[0], log_probs, 0.0)
        return log_probs[None, :]

    return jax.shard_map(device_step, mesh=mesh, in_specs=in_specs, out_specs=rows, check_vma=False)
```

```python
import functools

import jax
import jax.numpy as jnp
from jax import lax
from jax.experimental import pallas as pl
from jax.experimental.pallas import tpu as pltpu
from jax.sharding import PartitionSpec as P

EPS = 1e-6
ROPE_BASE = 10000.0
LOG2E = 1.4426950408889634
HD = 128
NH = 5
NEG = -1e30
BF, F32 = jnp.bfloat16, jnp.float32
ANY = pl.BlockSpec(memory_space=pl.ANY)
VMEM = pl.BlockSpec(memory_space=pltpu.VMEM)
DMA = pltpu.SemaphoreType.DMA
MESH = pl.DeviceIdType.MESH
NT = (((1,), (1,)), ((), ()))


PLAN = (
    "z00Q00-------z01/k00Q01-------z02/Q02-------z03x00/k01A00k02",
    "---o00--o04/z30A01---o01x01--o05o10/A02---o02--o06x02o11/o03",
    "o14o07o20x03T00-----o12o15---o21---o13-----o16s00-----o22s04",
    "/T01z31o17-----o23s01---z32---s05-----z33x30-----s02/s06x31s",
    "03g00o24s10s07g01g04o25x32s14g02x33g05o26T02s11g03g06s15o27-",
    "----g07s12-----------s16s13-----g10/Q10-------s17g14g11s20/k",
    "30s24g15g12s21g16Q11g13g17-------k31s25/A11k32---o40s22/o44o",
    "41s26s23o45o42s27o46T11g20g24o43o47-----g21------g22-----g23",
    "g25s40-----s44/g26Q12g27/s41A12---o50--o54s42/o51o55s45s43o5",
    "2o56T12g40o53o57-----s46---g41--------s47g42g44s50-----g43/s",
    "54g45g46H01s51g47----s52----s53g50s55/g51s56g52H12s57g54g53-",
    "---g55----g56/g57H22/",
)
RADIX = {-5: (2, 3, 2, 3, 2), -3: (2, 7, 3), -2: (2, 3)}
GROUPS = ((0, 3), (3, 5))


def read_plan():
    text = "".join(PLAN)
    names = {"Q": "qkv", "A": "attn", "T": "tail", "H": "head"}
    plan, hooks, where = [], None, 0
    marks = iter(text)
    for mark in marks:
        if mark == "-":
            where += 1
        elif mark == "/":
            hooks = None
        elif mark.isupper():
            hooks, where = {}, -1
            plan.append((names[mark], int(next(marks)), int(next(marks)), hooks))
        else:
            at, k = int(next(marks)), int(next(marks))
            step = (mark, at // 3, at % 3, k // 4, k % 4)
            if hooks is None:
                plan.append(step)
            else:
                hooks.setdefault(where, []).append(step)
    return plan


class Rows:
    def __init__(self, buf, first):
        self.buf, self.first, self.at = buf, first, self

    def __getitem__(self, i):
        return self.buf.at[self.first + i]


def norm_rows(x, gain):
    x = x.astype(F32)
    inv = lax.rsqrt(jnp.mean(x * x, axis=-1, keepdims=True) + EPS)
    return (x * inv * gain).astype(BF)


def program(sizes, *refs):
    chunk, dim, hidden, vocab, scale = sizes
    half = chunk // 2
    unit = half // 4
    (xp, xr, tgt, again, mgain, fgain, cos, sin, wq, wk, wv, w_out, wg, wu, wd, wvoc) = refs[:16]
    (kvb, kvr, qb, og, og_last, pt, x1b, rr, rl, sr, sl, xg, wf, st_m, st_l, st_p) = refs[16:32]
    (va, vb, vc, vd, xs, lsem, ago_s, ago_r, agx_s, agx_r, rs_s, rs_r, kv_s, kv_r, wz_s, wz_r, wx_s, wx_r) = refs[32:]
    n_piece = 8
    piece = w_out.shape[1] // n_piece
    local = w_out.shape[1]

    z = lax.axis_index('model')
    r = lax.axis_index('resp')
    px = lax.axis_index('prompts')
    y, core = lax.div(r, 2), lax.rem(r, 2)
    r_core, r_y, r_yc = y * 2 + (1 - core), (1 - y) * 2 + core, (1 - y) * 2 + (1 - core)
    others = (r, r_core, r_y, r_yc)
    nx = 1 - px
    ending = []
    free = None

    def remote(src, dst, sems, at, dev):
        slot = 0
        for digit, base in zip(at, RADIX[-len(at)]):
            slot = slot * base + digit
        return pltpu.make_async_remote_copy(
            src, dst, sems[0].at[slot], sems[1].at[slot], device_id=dev, device_id_type=MESH)

    def when(cond, body):
        if cond is free:
            body()
        else:
            pl.when(cond)(body)

    def send(cond, *args):
        copy = lambda: remote(*args)
        when(cond, (lambda: copy().wait_send()) if ending else (lambda: copy().start()))

    def recv(cond, ref, *args):
        if not ending:
            when(cond, lambda: remote(ref, ref, *args).wait_recv())

    right, left = (px, z + 1, r), (px, z - 1, r)
    to_y, to_core, to_x = (px, z, r_y), (px, z, r_core), (nx, z, r)


    def gather(k, block, sems, at, own=None):
        sides = ((z - k, 0, right), (3 - z - k, 1, left))
        for room, side, to in sides:
            j = lax.rem(z + 4 + (2 * side - 1) * k, 4)
            src = own if own is not None and k == 0 else block(j)
            if k:
                recv(room >= 0, src, sems, at + (k - 1, side), to)
            if k < 3:
                ahead = z <= 2 if side == 0 else z >= 1
                send((room >= 0) & ahead, src, block(j), sems, at + (k, side), to)

    def heads_out(l, c, g, j):
        return (og_last if g else og).at[l * 3 + c, j]

    def step_ago(l, c, g, k):
        gather(k, lambda j: heads_out(l, c, g, j), (ago_s, ago_r), (l, c, g))

    def rows_at(g, j):
        return pl.ds(pl.multiple_of(g * half + j * unit, 16), unit)

    def step_agx(l, c, g, k):
        gather(k, lambda j: xg.at[l * 3 + c, rows_at(g, j)], (agx_s, agx_r), (l, c, g))

    def load(*pairs):
        copies = [pltpu.make_async_copy(s, d, lsem.at[i]) for i, (s, d) in enumerate(pairs)]
        for cp in copies:
            cp.start()
        for cp in copies:
            cp.wait()

    def add_rows(dst, *srcs):
        def body(i, carry):
            sl_ = pl.ds(pl.multiple_of(i * 16, 16), 16)
            total = srcs[0][sl_, :]
            for s in srcs[1:]:
                total = total + s[sl_, :]
            dst[sl_, :] = total
            return carry

        lax.fori_loop(0, unit // 16, body, 0)

    def step_rs(l, c, g, k):
        part, r_in, l_in, r_out, l_out = (lambda j: pt.at[l * 3 + c, rows_at(g, j)]), *(Rows(buf, ((l * 3 + c) * 2 + g) * 3) for buf in (rr, rl, sr, sl))
        sems, at = (rs_s, rs_r), (l, c, g)
        if k < 3:
            send(z == 0, part(3 - k), r_in.at[k], sems, at + (k, 0), right)
            send(z == 3, part(k), l_in.at[k], sems, at + (k, 1), left)
        if k == 1:
            for cond, side, far, src, out, to in ((z == 1, 0, 3, r_in, r_out, right), (z == 2, 1, 0, l_in, l_out, left)):
                recv(cond, src.at[0], sems, at + (0, side), to)
                if not ending:
                    @pl.when(cond)
                    def _():
                        load((part(far), va), (src.at[0], vb))
                        add_rows(va, va, vb)
                        load((va, out.at[0]))
                send(cond, out.at[0], src.at[1], sems, at + (1, side), to)
        elif k == 2:
            mid = (z >= 1) & (z <= 2)
            sides = ((0, r_in, r_out, right), (1, l_in, l_out, left))
            for side, src, out, to in sides:
                recv(mid, src.at[1], sems, at + (1, side), to)
            if not ending:
                @pl.when(mid)
                def _():
                    load((part(z + 1), va), (r_in.at[1], vb), (part(z - 1), vc), (l_in.at[1], vd))
                    add_rows(va, va, vb)
                    add_rows(vc, vc, vd)
                    load((va, r_out.at[1]), (vc, l_out.at[1]))
            for side, src, out, to in sides:
                send(mid, out.at[1], src.at[2], sems, at + (2, side), to)
        elif k == 3 and not ending:
            ends = ((2, z >= 1, r_in.at[2], vb, right), (3, z <= 2, l_in.at[2], vc, left))
            for idx, cond, src, dst, to in ends:
                recv(cond, src, sems, at + (2, idx - 2), to)
            copies = [pltpu.make_async_copy(part(z), va, lsem.at[0]), pltpu.make_async_copy(x1b.at[(l * 3 + c) * 2 + g], xs, lsem.at[1])]
            for cp in copies:
                cp.start()
            for idx, cond, src, dst, _ in ends:
                @pl.when(cond)
                def _():
                    one = pltpu.make_async_copy(src, dst, lsem.at[idx])
                    one.start()
                    one.wait()

                @pl.when(jnp.logical_not(cond))
                def _():
                    dst[...] = jnp.zeros(dst.shape, F32)
            for cp in copies:
                cp.wait()

            def body(i, carry):
                s_ = pl.ds(pl.multiple_of(i * 16, 16), 16)
                total = va[s_, :] + (vb[s_, :] + vc[s_, :])
                xs[s_, :] = (xs[s_, :].astype(F32) + total).astype(BF)
                return carry

            lax.fori_loop(0, unit // 16, body, 0)
            load((xs, xg.at[l * 3 + c, rows_at(g, z)]))

    def step_kv(l, c, g, k):
        slots, sems = [kvr.at[l, i] for i in range(3)], (kv_s, kv_r)
        if k == 0:
            send(free, kvb.at[l, 0], slots[1], sems, (l, 1), to_y)
            send(free, kvb.at[l, 0], slots[0], sems, (l, 0), to_core)
        elif k == 1:
            recv(free, slots[1], sems, (l, 1), to_y)
            send(free, slots[1], slots[2], sems, (l, 2), to_core)
        else:
            recv(free, slots[0], sems, (l, 0), to_core)
            recv(free, slots[2], sems, (l, 2), to_core)

    def rows_of(j, rr_, xx):
        return pl.ds(pl.multiple_of(j * local + (xx * 4 + rr_) * piece, 16), piece)

    def step_wz(l, c, g, k):
        own = w_out.at[l, pl.ds(pl.multiple_of((px * 4 + r) * piece, 16), piece), :]
        gather(k, lambda j: wf.at[l, rows_of(j, r, px), :], (wz_s, wz_r), (l,), own)

    def step_wx(l, c, g, k):
        for s in range(3):
            j = lax.rem(z + 1 + s, 4)

            def push(i, place, to):
                at = wf.at[l, rows_of(j, *place), :]
                send(free, at, at, (wx_s, wx_r), (l, i, s), to)

            def pull(i, place, to):
                recv(free, wf.at[l, rows_of(j, *place), :], (wx_s, wx_r), (l, i, s), to)

            here, over_y, over_x, over_xy = (r, px), (r_y, px), (r, nx), (r_y, nx)
            if k == 0:
                push(0, here, to_y)
                push(1, here, to_x)
            elif k == 1:
                pull(0, over_y, to_y)
                push(2, over_y, to_x)
            elif k == 2:
                pull(1, over_x, to_x)
                pull(2, over_xy, to_x)
                for i, place in enumerate((here, over_y, over_x, over_xy)):
                    push(3 + i, place, to_core)
            else:
                for i, place in enumerate(((r_core, px), (r_yc, px), (r_core, nx), (r_yc, nx))):
                    pull(3 + i, place, to_core)

    steps = {"o": step_ago, "g": step_agx, "s": step_rs, "k": step_kv, "z": step_wz, "x": step_wx}

    def emit(item):
        steps[item[0]](*item[1:])

    def pre(hooks):
        for item in hooks.get(-1, []):
            emit(item)

    def loop(n, body, hooks, base):
        begin = 0
        for i in range(n):
            if hooks.get(base + i) or i == n - 1:
                lax.fori_loop(begin, i + 1, lambda k, carry: (body(k), carry)[1], 0)
                begin = i + 1
                for item in hooks.get(base + i, []):
                    emit(item)

    def steps_of(n, body, hooks, base):
        for i in range(n):
            body(i)
            for item in hooks.get(base + i, []):
                emit(item)


    def load_x(l, c, x_vm, sem, first=0):
        rows = pl.ds(first, x_vm.shape[0])
        if l:
            src = xg.at[(l - 1) * 3 + c, rows]
        elif c:
            src = xr.at[0, pl.ds((c - 1) * chunk, chunk)]
        else:
            src = xp
        copy = pltpu.make_async_copy(src, x_vm, sem.at[0])
        copy.start()
        return copy

    def norm_all(src, dst, gain):
        rows = src.shape[0]

        def body(i, carry):
            s_ = pl.ds(pl.multiple_of(i * 32, 32), 32)
            dst[s_, :] = norm_rows(src[s_, :], gain)
            return carry

        lax.fori_loop(0, rows // 32, body, 0)

    def task_qkv(l, c, hooks):
        with_q = not (l == 1 and c == 0)
        kinds = (wk, wq, wv) if with_q else (wk, wv)
        n_w = NH * len(kinds)

        def scoped(x_vm, w_vm, o_vm, cs_vm, x_sems, w_sems, o_sems, c_sems):
            c_copies = [pltpu.make_async_copy(src.at[c], cs_vm.at[i], c_sems.at[i]) for i, src in enumerate((cos, sin))]
            w_copies = [pltpu.make_async_copy(w.at[l], w_vm.at[NH * i:NH * (i + 1)], w_sems.at[i]) for i, w in enumerate(kinds)]
            for cp in c_copies + w_copies:
                cp.start()
            pre(hooks)
            load_x(l, c, x_vm, x_sems).wait()
            norm_all(x_vm, x_vm, again[l:l + 1, :])
            for cp in c_copies + w_copies:
                cp.wait()
            cs, sn = cs_vm[0], cs_vm[1]

            def rope(part):
                return part * cs + pltpu.roll(part, HD // 2, 1) * sn

            def pair(i, ropes):
                both = jnp.concatenate([w_vm[i], w_vm[i + 1]], axis=1)
                full = jnp.dot(x_vm[...], both, preferred_element_type=F32)
                for n, with_rope in enumerate(ropes):
                    part = full[:, n * HD:(n + 1) * HD]
                    o_vm[i + n] = (rope(part) if with_rope else part).astype(BF)

            n_rope = n_w - NH

            steps_of(n_rope // 2, lambda i: pair(2 * i, (True, True)), hooks, 0)
            first = n_rope
            if n_rope % 2:
                pair(n_rope - 1, (True, False))
                first = n_rope + 1

            steps_of(2, lambda i: pair(first + 2 * i, (False, False)), hooks, 5)
            if first + 4 < n_w:
                o_vm[n_w - 1] = jnp.dot(x_vm[...], w_vm[n_w - 1], preferred_element_type=F32).astype(BF)
            outs = [(o_vm.at[0:NH], kvb.at[l, c, 0:NH]), (o_vm.at[n_w - NH:n_w], kvb.at[l, c, NH:2 * NH])]
            if with_q:
                outs.append((o_vm.at[NH:2 * NH], qb.at[l, c]))
            o_copies = [pltpu.make_async_copy(s, d, o_sems.at[i]) for i, (s, d) in enumerate(outs)]
            for cp in o_copies:
                cp.start()
            for cp in o_copies:
                cp.wait()

        pl.run_scoped(
            scoped, pltpu.VMEM((chunk, dim), BF), pltpu.VMEM((n_w, dim, HD), BF), pltpu.VMEM((n_w, chunk, HD), BF),
            pltpu.VMEM((2, chunk, HD), F32), DMA((1,)), DMA((3,)), DMA((3,)), DMA((2,)),
        )

    def task_attn(l, c, hooks):
        blocks = [kvb.at[l, 0], kvr.at[l, 0], kvr.at[l, 1], kvr.at[l, 2]] + [kvb.at[l, i] for i in range(1, c + 1)]
        n_blk = len(blocks)
        if c == 0:
            plan = [(0, "causal")] + [(m, "if") for m in (1, 2, 3)]
        else:
            plan = [(b, "causal" if b == n_blk - 1 else "full") for b in range(n_blk)]
        coef = scale * LOG2E

        def scoped(q_vm, kv_vm, s_vm, mx_vm, l_vm, acc_vm, o_vm, sems):
            copies = [pltpu.make_async_copy(qb.at[l, c], q_vm, sems.at[n_blk])]
            copies += [pltpu.make_async_copy(src, kv_vm.at[b], sems.at[b]) for b, src in enumerate(blocks)]
            pre(hooks)
            for cp in copies:
                cp.start()
            for cp in copies:
                cp.wait()

            def head_body(h):
                mx_vm[...] = jnp.full(mx_vm.shape, -jnp.inf, F32)
                l_vm[...] = jnp.zeros(l_vm.shape, F32)
                acc_vm[...] = jnp.zeros(acc_vm.shape, F32)

                def scores(b, causal):
                    s = lax.dot_general(q_vm[h], kv_vm[b, h], NT, preferred_element_type=F32)
                    if causal:
                        row = lax.broadcasted_iota(jnp.int32, s.shape, 0)
                        col = lax.broadcasted_iota(jnp.int32, s.shape, 1)
                        s = jnp.where(row >= col, s, -jnp.inf)
                    s_vm[:, b * chunk:(b + 1) * chunk] = s
                    top = mx_vm[...]
                    for t in range(chunk // HD):
                        top = jnp.maximum(top, s[:, t * HD:(t + 1) * HD])
                    mx_vm[...] = top

                def mix(b, m):
                    p = jnp.exp2((s_vm[:, b * chunk:(b + 1) * chunk] - m) * coef)
                    total = l_vm[...]
                    for t in range(chunk // HD):
                        total = total + p[:, t * HD:(t + 1) * HD]
                    l_vm[...] = total
                    acc_vm[...] += jnp.dot(p.astype(BF), kv_vm[b, NH + h], preferred_element_type=F32)

                for b, kind in plan:
                    if kind == "if":
                        pl.when(others[b] < r)(functools.partial(scores, b, False))
                    else:
                        scores(b, kind == "causal")
                m = jnp.max(mx_vm[...], axis=1, keepdims=True)
                for b, kind in plan:
                    if kind == "if":
                        pl.when(others[b] < r)(functools.partial(mix, b, m))
                    else:
                        mix(b, m)
                out = (acc_vm[...] / jnp.sum(l_vm[...], axis=1, keepdims=True)).astype(BF)
                o_vm[:, pl.ds(pl.multiple_of(h * HD, HD), HD)] = out

            for g, (first, end) in enumerate(GROUPS):
                lax.fori_loop(first, end, lambda h, carry: (head_body(h), carry)[1], 0)
                out_copy = pltpu.make_async_copy(o_vm.at[:, first * HD:end * HD], heads_out(l, c, g, z), sems.at[0])
                out_copy.start()
                out_copy.wait()
                for item in hooks.get(end - 1, []):
                    emit(item)

        pl.run_scoped(
            scoped, pltpu.VMEM((NH, chunk, HD), BF), pltpu.VMEM((n_blk, 2 * NH, chunk, HD), BF),
            pltpu.VMEM((chunk, n_blk * chunk), F32), pltpu.VMEM((chunk, HD), F32), pltpu.VMEM((chunk, HD), F32),
            pltpu.VMEM((chunk, HD), F32), pltpu.VMEM((chunk, NH * HD), BF), DMA((n_blk + 1,)),
        )

    def task_tail(l, c, hooks):
        full_blocks, rest = hidden // 256, hidden % 256

        def scoped(o_vm, x_vm, wo_vm, wg_vm, wu_vm, wd_vm, acc_vm, in_vm, o_sems, x_sems, wo_sems, w_sems, p_sems):
            wo_copies = [pltpu.make_async_copy(
                w_out.at[l], wo_vm.at[pl.ds(pl.multiple_of(z * local, 128), local), :], wo_sems.at[0])]
            for s in (1, 2, 3):
                rows = pl.ds(pl.multiple_of(lax.rem(z + s, 4) * local, 128), local)
                wo_copies.append(pltpu.make_async_copy(wf.at[l, rows, :], wo_vm.at[rows, :], wo_sems.at[s]))
            for cp in wo_copies:
                cp.start()
            x_copy = load_x(l, c, x_vm, x_sems)
            w_copies = [pltpu.make_async_copy(s.at[l], d, w_sems.at[i]) for i, (s, d) in enumerate(((wg, wg_vm), (wu, wu_vm), (wd, wd_vm)))]
            for cp in w_copies:
                cp.start()
            pre(hooks)
            o_copies = []
            for j in range(4):
                for g, (first, end) in enumerate(GROUPS):
                    cols = o_vm.at[:, j * local + first * HD:j * local + end * HD]
                    o_copies.append(pltpu.make_async_copy(heads_out(l, c, g, j), cols, o_sems.at[j, g]))
            for cp in o_copies:
                cp.start()
            for cp in wo_copies + o_copies:
                cp.wait()
            wide = dim // 5

            def out_body(i):
                cols = pl.ds(i * wide, wide)
                acc_vm[:, cols] = jnp.dot(o_vm[...], wo_vm[:, cols], preferred_element_type=F32)

            steps_of(5, out_body, hooks, 0)
            x_copy.wait()
            gain = mgain[l:l + 1, :]

            def finish(i, carry):
                s_ = pl.ds(pl.multiple_of(i * 32, 32), 32)
                x1 = (x_vm[s_, :].astype(F32) + acc_vm[s_, :]).astype(BF)
                x_vm[s_, :] = x1
                o_vm[s_, :] = norm_rows(x1, gain)
                return carry

            lax.fori_loop(0, chunk // 32, finish, 0)
            x1_copies = [
                pltpu.make_async_copy(
                    x_vm.at[pl.ds(pl.multiple_of(g * half + z * unit, 16), unit), :], x1b.at[(l * 3 + c) * 2 + g], x_sems.at[g])
                for g in range(2)
            ]
            for cp in x1_copies:
                cp.start()
            w_copies[0].wait()
            w_copies[1].wait()

            def gate_up(rows, cols):
                gate = lax.dot_general(o_vm[...], wg_vm[rows, :], NT, preferred_element_type=F32)
                up = lax.dot_general(o_vm[...], wu_vm[rows, :], NT, preferred_element_type=F32)
                in_vm[:, cols] = (jax.nn.silu(gate) * up).astype(BF)

            def gate_body(i):
                s_ = pl.ds(i * 256, 256)
                gate_up(s_, s_)

            steps_of(full_blocks, gate_body, hooks, 5)
            if rest:
                s_ = pl.ds(full_blocks * 256, rest)
                gate_up(s_, s_)
            w_copies[2].wait()

            for cp in x1_copies:
                cp.wait()
            for g in range(2):
                top = g * half

                def down_body(i):
                    cols = pl.ds(i * wide, wide)
                    acc_vm[top:top + half, cols] = jnp.dot(in_vm[top:top + half, :], wd_vm[:, cols], preferred_element_type=F32)

                steps_of(5, down_body, {}, 0)
                p_copy = pltpu.make_async_copy(acc_vm.at[top:top + half], pt.at[l * 3 + c, pl.ds(top, half)], p_sems.at[g])
                p_copy.start()
                p_copy.wait()
                for item in hooks.get(9 + full_blocks + 5 * g, []):
                    emit(item)

        pl.run_scoped(
            scoped, pltpu.VMEM((chunk, dim), BF), pltpu.VMEM((chunk, dim), BF), pltpu.VMEM((4 * local, dim), BF),
            pltpu.VMEM((hidden, dim), BF), pltpu.VMEM((hidden, dim), BF), pltpu.VMEM((hidden, dim), BF),
            pltpu.VMEM((chunk, dim), F32), pltpu.VMEM((chunk, hidden), BF),
            DMA((4, 2)), DMA((2,)), DMA((4,)), DMA((3,)), DMA((2,)),
        )

    def task_head(mode, c, hooks):
        wide = 1024
        n_steps = vocab // (2 * wide)
        rows = half if mode else chunk
        begin = (mode - 1) * half if mode else 0
        out = c - 1

        def scoped(h_vm, w_vm, a_vm, b_vm, mx_vm, sum_vm, pick_vm, want_vm, x_sems, w_sems):
            def fetch(i, slot):
                cols = pl.ds(pl.multiple_of(i * 2 * wide, 2 * wide), 2 * wide)
                return pltpu.make_async_copy(wvoc.at[:, cols], w_vm.at[slot], w_sems.at[slot])

            fetch(0, 0).start()
            pre(hooks)
            load_x(2, c, h_vm, x_sems, begin).wait()
            norm_all(h_vm, h_vm, fgain[...])
            want_vm[...] = tgt[out, begin:begin + rows, :]
            b_vm[...] = jnp.full(b_vm.shape, NEG, F32)
            mx_vm[...] = jnp.full(mx_vm.shape, NEG, F32)
            sum_vm[...] = jnp.zeros(sum_vm.shape, F32)
            pick_vm[...] = jnp.zeros(pick_vm.shape, F32)

            def narrow(x, op):
                while x.shape[1] > HD:
                    mid = x.shape[1] // 2
                    x = op(x[:, :mid], x[:, mid:])
                return x

            def fold(src, first, at):
                block, old = src[at, :], mx_vm[at, :]
                top = jnp.maximum(old, narrow(block, jnp.maximum))
                terms = jnp.exp(block - jnp.concatenate([top] * (wide // HD), axis=1))
                hit = want_vm[at, :] - first == lax.broadcasted_iota(jnp.int32, block.shape, 1)
                mx_vm[at, :] = top
                sum_vm[at, :] = sum_vm[at, :] * jnp.exp(old - top) + narrow(terms, jnp.add)
                pick_vm[at, :] += narrow(jnp.where(hit, block, 0.0), jnp.add)

            def folds(src, first, lo, n):
                for i in range(n // 32):
                    fold(src, first, pl.ds(lo + i * 32, 32))

            def phase(dst, slot, col, src, first):
                n_sub = wide // 256
                n = rows // n_sub
                for sub in range(n_sub):
                    lo = sub * 256
                    dst[:, lo:lo + 256] = jnp.dot(
                        h_vm[...], w_vm[slot, :, col + lo:col + lo + 256], preferred_element_type=F32)
                    folds(src, first, sub * n, n)

            def body(i):
                slot = lax.rem(i, 2)

                @pl.when(i + 1 < n_steps)
                def _():
                    fetch(i + 1, 1 - slot).start()

                fetch(i, slot).wait()
                base = i * 2 * wide
                phase(a_vm, slot, 0, b_vm, jnp.where(i == 0, vocab * 8, base - wide))
                phase(b_vm, slot, wide, a_vm, base)

            loop(n_steps, body, hooks, 0)
            last_fold = lambda i, carry: (fold(b_vm, vocab - wide, pl.ds(pl.multiple_of(i * 32, 32), 32)), carry)[1]
            lax.fori_loop(0, rows // 32, last_fold, 0)
            top = jnp.max(mx_vm[...], axis=1, keepdims=True)
            total = jnp.sum(sum_vm[...] * jnp.exp(mx_vm[...] - top), axis=1, keepdims=True)
            pick = jnp.sum(pick_vm[...], axis=1, keepdims=True)
            st_m[out, begin:begin + rows, :] = jnp.broadcast_to(top, (rows, HD))
            st_l[out, begin:begin + rows, :] = jnp.broadcast_to(total, (rows, HD))
            st_p[out, begin:begin + rows, :] = jnp.broadcast_to(pick, (rows, HD))

        pl.run_scoped(
            scoped, pltpu.VMEM((rows, dim), BF), pltpu.VMEM((2, dim, 2 * wide), BF),
            pltpu.VMEM((rows, wide), F32), pltpu.VMEM((rows, wide), F32), pltpu.VMEM((rows, HD), F32),
            pltpu.VMEM((rows, HD), F32), pltpu.VMEM((rows, HD), F32), pltpu.VMEM((rows, 1), jnp.int32), DMA((1,)), DMA((2,)),
        )

    tasks = {"qkv": task_qkv, "attn": task_attn, "tail": task_tail, "head": task_head}

    barrier = pltpu.get_barrier_semaphore()

    def greet(dev):
        pl.semaphore_signal(barrier, inc=1, device_id=dev, device_id_type=MESH)

    for dev in (to_core, to_y, to_x):
        greet(dev)
    pl.when(z <= 2)(lambda: greet(right))
    pl.when(z >= 1)(lambda: greet(left))
    pl.semaphore_wait(barrier, 3 + lax.div(z + 2, 3) + lax.div(5 - z, 3))

    plan = read_plan()
    for entry in plan:
        if entry[0] in tasks:
            tasks[entry[0]](*entry[1:])
        else:
            emit(entry)
    ending.append(True)
    for entry in plan:
        for item in (sum(entry[-1].values(), []) if entry[0] in tasks else [entry]):
            emit(item)


def solution(mesh):
    row_axes = ('prompts', 'resp')
    rows, whole, second, third = P(row_axes), P(), P(None, 'model'), P(None, None, 'model')
    in_specs = (rows, rows, rows, rows, whole, third, third, third, second, whole, third, third, second, whole, second)
    groups = mesh.shape['resp']

    def device_step(x_prompt, x_resp, targets, resp_lens, attn_gain, w_query, w_key, w_value, w_out, mlp_gain, w_gate, w_up, w_down, final_gain, w_vocab):
        chunk, dim = x_prompt.shape
        resp_len = x_resp.shape[1]
        prompt_len = chunk * groups
        n_l = w_query.shape[0]
        hidden = w_gate.shape[2]
        vocab = w_vocab.shape[1]
        local = w_out.shape[1] * HD
        z = lax.axis_index('model')
        r = lax.axis_index('resp')
        heads_first = lambda w: jnp.transpose(w, (0, 2, 1, 3))

        tok_pos = jnp.concatenate([r * chunk + jnp.arange(chunk), prompt_len + jnp.arange(resp_len)])
        half = HD // 2
        frequency = ROPE_BASE ** (-jnp.arange(half, dtype=F32) / half)
        angles = tok_pos.astype(F32)[:, None] * frequency
        cos, sin = jnp.cos(angles), jnp.sin(angles)
        n_resp = resp_len // chunk
        n_c = 1 + n_resp
        cos = jnp.concatenate([cos, cos], axis=1).reshape(n_c, chunk, HD)
        sin = jnp.concatenate([-sin, sin], axis=1).reshape(n_c, chunk, HD)
        tgt = (targets[0] - z * vocab).reshape(n_resp, chunk, 1)
        unit = chunk // 8

        sds = jax.ShapeDtypeStruct
        out_shape = [
            sds((n_l, n_c, 2 * NH, chunk, HD), BF), sds((n_l, 3, 2 * NH, chunk, HD), BF), sds((n_l, n_c, NH, chunk, HD), BF),
            sds((n_l * n_c, 4, chunk, 3 * HD), BF), sds((n_l * n_c, 4, chunk, 2 * HD), BF), sds((n_l * n_c, chunk, dim), F32), sds((n_l * n_c * 2, unit, dim), BF),
        ] + [sds((n_l * n_c * 6, unit, dim), F32)] * 4 + [
            sds((n_l * n_c, chunk, dim), BF), sds((n_l, 4 * local, dim), BF),
        ] + [sds((n_resp, chunk, HD), F32)] * 3
        outs = pl.pallas_call(
            functools.partial(program, (chunk, dim, hidden, vocab, HD ** -0.5)),
            out_shape=out_shape,
            in_specs=[ANY, ANY, VMEM, VMEM, VMEM, VMEM] + [ANY] * 10,
            out_specs=[ANY] * 13 + [VMEM] * 3,
            scratch_shapes=[pltpu.VMEM((unit, dim), F32)] * 4 + [pltpu.VMEM((unit, dim), BF), DMA((4,))] + [DMA((72,))] * 6
            + [DMA((6,))] * 2 + [DMA((42,))] * 4,
            compiler_params=pltpu.CompilerParams(collective_id=0, has_side_effects=True, vmem_limit_bytes=67043328),
            name="decoder",
        )(x_prompt, x_resp, tgt, attn_gain, mlp_gain, final_gain[None], cos, sin, heads_first(w_query), heads_first(w_key), heads_first(w_value), w_out.reshape(n_l, local, dim), jnp.transpose(w_gate, (0, 2, 1)), jnp.transpose(w_up, (0, 2, 1)), w_down, w_vocab)
        stats = jnp.stack([s[:, :, 0].reshape(resp_len) for s in outs[13:]])
        stats = lax.all_gather(stats, 'model', axis=0)
        row_max = jnp.max(stats[:, 0], axis=0)
        exp_total = jnp.sum(stats[:, 1] * jnp.exp(stats[:, 0] - row_max), axis=0)
        picked = jnp.sum(stats[:, 2], axis=0)
        log_probs = picked - row_max - jnp.log(exp_total)
        log_probs = jnp.where(jnp.arange(resp_len) < resp_lens[0], log_probs, 0.0)
        return log_probs[None, :]

    return jax.shard_map(device_step, mesh=mesh, in_specs=in_specs, out_specs=rows, check_vma=False)
```
